32 devices in a mesh: facet: 16 (over z, x, core), col: 2 (over y).
Axes of the slice: x: 2, y: 2, z: 4, core: 2. Of those that a mesh axis runs over, the one named last changes fastest.
Arguments:
- facet_strips: bfloat16 [16, 2, 8192, 128], P('facet', None, 'col'), may hold values from -6 to 6
- facet_offsets: int32 [16, 2], P('facet'), may hold values from 0 to 65535
- column_offsets: int32 [2], P('col'), may hold values from 0 to 65535
- row_offsets: int32 [1], replicated, may hold values from 0 to 65535
- tile_lists: int32 [2, 16, 8], P('col', 'facet'), may hold values from 0 to 63
- tile_counts: int32 [2, 16], P('col', 'facet'), may hold values from 1 to 8, 64 in all within a row
- uv_index: int32 [2, 16, 8, 2, 1024], P('col', 'facet'), may hold values from 0 to 4095
Outputs:
- visibilities: float32 [2, 16, 8, 2, 1024], P('col', 'facet')
The draws below stay inside these ranges and needn't reach their ends.
Inputs may be any that keep to these rules, and one draw needn't show every extreme that they name: `tile_counts`: each column has an owner whose count is exactly 8.
All inputs are finite; a program needn't handle non-finite values. No bound on the sum of `tile_counts` on one device may be relied on, other than what follows from the above.
Results may differ from the reference program's by a relative error of at most 0.0058.
Values may be sent and summed in bfloat16 or wider, within the bound.
No kernel may reach another device: no remote copies, remote signals or barrier semaphores. Data moves between devices by JAX's collectives and lax.ppermute only.
A program may use at most 64 MiB of HBM per device.

```python
import math
import jax
import jax.numpy as jnp
import numpy as np
from jax import lax

L = 8192
W = 128
S = 256
TILE = 32
NTOT = 65536
UV_STEPS = 4096
VIS = 1024
CAP = 8
ROWS = 1
FACETS = 16
COLS = 2
OWNERS = 16
TILE_IDS = 64


def touch_ends(array, key, least, largest):
    place = [jax.random.randint(jax.random.fold_in(key, axis), (), 0, length) for axis, length in enumerate(array.shape)]
    widest = array.shape.index(max(array.shape))
    next_to = place[:widest] + [(place[widest] + 1) % array.shape[widest]] + place[widest + 1:]
    return array.at[tuple(place)].set(least).at[tuple(next_to)].set(largest)


def block_levels(stream_key, dims, pieces, smallest, high):
    def one(dim, blocks):
        draws = jax.random.uniform(jax.random.fold_in(jax.random.fold_in(stream_key, 6), dim), (blocks,), jnp.float32, smallest / len(pieces), high / len(pieces))
        return jnp.repeat(jnp.exp(draws), dims[dim] // blocks).reshape((-1,) + (1,) * (len(dims) - dim - 1))

    gain = one(*pieces[0])
    for cut in pieces[1:]:
        gain = gain * one(*cut)
    return gain


def length_profile(count, total, bound, lean):
    weights = [(1 << 20) // math.isqrt(standing ** lean) + 1 for standing in range(2, count + 1)]
    spare, counts = total - bound - (count - 1), [1] * (count - 1)
    while spare > 0:
        movable = [i for i in range(count - 1) if counts[i] < bound]
        pool, remaining = sum([weights[i] for i in movable]), spare
        for i in movable:
            addition = min(bound - counts[i], max(1, remaining * weights[i] // pool), spare)
            counts[i] = counts[i] + addition
            spare = spare - addition
    return np.array([bound] + counts)


def ragged(own_key, number_of, total, bound, lean):
    if number_of == 2:
        one = jax.random.randint(own_key, (), max(1, total - bound), min(bound, total - 1) + 1)
        return jnp.stack([one, total - one])
    tallies = jnp.asarray(length_profile(number_of, total, bound, lean), jnp.int32)
    twos = (number_of - 1) // 2
    source_of, taker = tallies[1:1 + 2 * twos:2], tallies[2:2 + 2 * twos:2]
    room = jnp.minimum(source_of - 1, bound - taker)
    moved = jax.random.randint(jax.random.fold_in(own_key, 1), (twos,), 0, 1 << 20) % (room + 1)
    tallies = tallies.at[1:1 + 2 * twos:2].set(source_of - moved).at[2:2 + 2 * twos:2].set(taker + moved)
    return tallies[jax.random.permutation(jax.random.fold_in(own_key, 2), number_of)]


def centred(rng, dims, width, bound, pieces=(), kind=jnp.bfloat16):
    result = jax.random.normal(rng, dims, jnp.float32) * width
    if len(pieces) > 0:
        result = block_levels(rng, dims, pieces, -0.22, 0.18) * result
    return jnp.clip(result, min=-bound, max=bound).astype(kind)


def setup_inputs(seed: int = 0) -> dict:
    keys = jax.random.split(jax.random.key(seed), 8)
    facet_strips = centred(keys[0], (FACETS, 2, L, W), 1.0, 6.0, ((0, 16), (2, 2)))
    facet_offsets = touch_ends(jax.random.randint(keys[1], (FACETS, 2), 0, NTOT), jax.random.fold_in(keys[1], 1), 0, NTOT - 1).astype(jnp.int32)
    column_offsets = jax.random.randint(keys[2], (COLS,), 0, NTOT).astype(jnp.int32)
    row_offsets = jax.random.randint(keys[3], (ROWS,), 0, NTOT).astype(jnp.int32)
    tile_lists = touch_ends(jax.random.randint(keys[4], (COLS, OWNERS, CAP), 0, TILE_IDS), jax.random.fold_in(keys[4], 1), 0, TILE_IDS - 1).astype(jnp.int32)
    tile_counts = jax.vmap(lambda own: ragged(own, OWNERS, OWNERS * CAP // 2, CAP, 2))(jax.random.split(keys[5], COLS)).reshape((COLS, OWNERS)).astype(jnp.int32)
    uv_index = touch_ends(jax.random.randint(keys[6], (COLS, OWNERS, CAP, 2, VIS), 0, UV_STEPS), jax.random.fold_in(keys[6], 1), 0, UV_STEPS - 1).astype(jnp.int32)
    return {"facet_strips": facet_strips, "facet_offsets": facet_offsets, "column_offsets": column_offsets, "row_offsets": row_offsets, "tile_lists": tile_lists, "tile_counts": tile_counts, "uv_index": uv_index}


def mod_product(first, second):
    high = first // 256
    low = first % 256
    return (high * (second * 256 % NTOT) + low * second) % NTOT

def phase_parts(row_start, row_count, row_step, col_start, col_count, col_step):
    left_side = ((row_start + row_step * jnp.arange(row_count, dtype=jnp.int32)) % NTOT)[:, None]
    right_side = ((col_start + col_step * jnp.arange(col_count, dtype=jnp.int32)) % NTOT)[None, :]
    index = mod_product(left_side, right_side)
    angle = index.astype(jnp.float32) * (2.0 * math.pi / NTOT)
    return (jnp.cos(angle), jnp.sin(angle))

def left_operator(row_start, col_start, count):
    cosine, sine = phase_parts(row_start, S, NTOT // L, col_start, count, 1)
    upper = jnp.concatenate([cosine, sine], axis=1)
    lower = jnp.concatenate([-sine, cosine], axis=1)
    return (jnp.concatenate([upper, lower], axis=0) * (1.0 / math.sqrt(L))).astype(jnp.bfloat16)

def right_operator(column_start, strip_start):
    cosine, sine = phase_parts(strip_start, W, 1, column_start, S, NTOT // S)
    table = jnp.stack([jnp.stack([cosine, -sine], axis=1), jnp.stack([sine, cosine], axis=1)])
    table = table * (1.0 / math.sqrt(W))
    return table.reshape(2, W, 2, S // TILE, TILE).astype(jnp.bfloat16)

def tile_terms(strip_rows, table):
    count = strip_rows.shape[0]
    shaped = strip_rows.reshape(count, 2, S // TILE, TILE, W).astype(jnp.float32)
    terms = jnp.einsum('rkapw,kwjbq->abrjpq', shaped, table.astype(jnp.float32), preferred_element_type=jnp.float32)
    return terms.reshape((S // TILE) ** 2, count, 2, TILE * TILE)

def select_tiles(flat_tiles, identity, live):
    slots = jnp.arange(identity.shape[0], dtype=jnp.int32)
    ids = jnp.arange(flat_tiles.shape[0], dtype=jnp.int32)
    onehot = ((identity[:, None] == ids[None, :]) & (slots[:, None] < live)).astype(jnp.bfloat16)
    return jnp.dot(onehot, flat_tiles, preferred_element_type=jnp.float32).astype(jnp.bfloat16)

def visibilities_of(chosen, uv_slots):
    slots = chosen.shape[0]
    tiles = chosen.astype(jnp.float32).reshape(slots, 2, TILE, TILE)
    pixels = jnp.arange(TILE, dtype=jnp.int32)
    factor = 2.0 * math.pi / UV_STEPS
    u_angle = (uv_slots[:, 0, None, :] * pixels[None, :, None] % UV_STEPS).astype(jnp.float32) * factor
    v_angle = (uv_slots[:, 1, None, :] * pixels[None, :, None] % UV_STEPS).astype(jnp.float32) * factor
    u_cos, u_sin = (jnp.cos(u_angle), jnp.sin(u_angle))
    v_cos, v_sin = (jnp.cos(v_angle), jnp.sin(v_angle))
    high = lax.Precision.HIGHEST
    real_mid = jnp.einsum('cpq,cqk->cpk', tiles[:, 0], v_cos, precision=high) - jnp.einsum('cpq,cqk->cpk', tiles[:, 1], v_sin, precision=high)
    imag_mid = jnp.einsum('cpq,cqk->cpk', tiles[:, 0], v_sin, precision=high) + jnp.einsum('cpq,cqk->cpk', tiles[:, 1], v_cos, precision=high)
    real_vis = lax.optimization_barrier(jnp.sum(u_cos * real_mid - u_sin * imag_mid, axis=1)) / TILE
    imag_vis = lax.optimization_barrier(jnp.sum(u_cos * imag_mid + u_sin * real_mid, axis=1)) / TILE
    return jnp.stack([real_vis, imag_vis], axis=1)

def reference(facet_strips, facet_offsets, column_offsets, row_offsets, tile_lists, tile_counts, uv_index):

    def facet_rows(index):
        flat = facet_strips[index].reshape(2 * L, W)
        parts = [jnp.dot(left_operator(row_offsets[r], facet_offsets[index, 0], L), flat, preferred_element_type=jnp.float32).astype(jnp.bfloat16) for r in range(ROWS)]
        return jnp.stack(parts)
    rows_all = lax.map(facet_rows, jnp.arange(FACETS, dtype=jnp.int32))
    scale = 1.0 / math.sqrt(FACETS)
    outputs = []
    for column in range(COLS):

        def add_facet(carry, index):
            table = right_operator(column_offsets[column], facet_offsets[index, 1])
            return (carry + tile_terms(rows_all[index], table) * scale, None)
        start = jnp.zeros(((S // TILE) ** 2, ROWS, 2, TILE * TILE), jnp.float32)
        total, unused = lax.scan(add_facet, start, jnp.arange(FACETS, dtype=jnp.int32))
        flat_tiles = total.astype(jnp.bfloat16).reshape((S // TILE) ** 2 * ROWS, 2 * TILE * TILE)

        def owner_vis(owner):
            chosen = select_tiles(flat_tiles, tile_lists[column, owner], tile_counts[column, owner])
            return visibilities_of(chosen.reshape(-1, 2, TILE * TILE), uv_index[column, owner])
        outputs.append(lax.map(owner_vis, jnp.arange(OWNERS, dtype=jnp.int32)))
    return jnp.stack(outputs)
```

```python
import functools
import math

import jax
import jax.numpy as jnp
from jax import lax
from jax.experimental import pallas as pl
from jax.experimental.pallas import tpu as pltpu
from jax.sharding import PartitionSpec as P

L = 8192
W = 128
S = 256
TILE = 32
NTOT = 65536
UV_STEPS = 4096
BF16 = jnp.bfloat16
F32 = jnp.float32
I32 = jnp.int32


def cos_sin(index):
    shifted = index + NTOT // 8
    quadrant = shifted >> 14
    rest = (shifted & (NTOT // 4 - 1)) - NTOT // 8
    x = rest.astype(F32) * (2.0 * math.pi / NTOT)
    y = x * x
    sine = x + x * (y * (-1.0 / 6 + y * (1.0 / 120 + y * (-1.0 / 5040 + y * (1.0 / 362880)))))
    cosine = 1.0 + y * (-0.5 + y * (1.0 / 24 + y * (-1.0 / 720 + y * (1.0 / 40320))))
    odd = (quadrant & 1) != 0
    first = jnp.where(odd, sine, cosine)
    second = jnp.where(odd, cosine, sine)
    return (
        jnp.where(((quadrant + 1) & 2) != 0, -first, first),
        jnp.where((quadrant & 2) != 0, -second, second),
    )


def mod_phase(first, second):
    return (first * second) & (NTOT - 1)


def along_kernel(facets, cols, chunk, scal, strip, out, held, table, total, sems):
    count = held.shape[1]
    blocks = count // W
    steps = count // chunk
    copies = []
    for n in range(steps):
        part = pl.ds(n * chunk, chunk)
        copies.append(pltpu.make_async_copy(strip.at[:, part], held.at[:, part], sems.at[n]))
        copies[n].start()
    row_start, col_start, across = scal[0], scal[1], scal[2]
    row = row_start + (NTOT // L) * lax.broadcasted_iota(I32, (S, W), 0)
    lane = lax.broadcasted_iota(I32, (S, W), 1)
    cos_in, sin_in = cos_sin(mod_phase(row, lane))
    cos_out, sin_out = cos_sin(mod_phase(row, col_start + W * lane))
    scale = 1.0 / math.sqrt(L)
    cos_out = cos_out * scale
    sin_out = sin_out * scale
    for n in range(steps):
        for local in range(chunk // W):
            a = n * (chunk // W) + local
            c = cos_out[:, a : a + 1]
            s = sin_out[:, a : a + 1]
            place = slice(local * W, (local + 1) * W)
            table[n % 2, 0:S, place] = (c * cos_in - s * sin_in).astype(BF16)
            table[n % 2, S : 2 * S, place] = (s * cos_in + c * sin_in).astype(BF16)
        copies[n].wait()
        part = slice(n * chunk, (n + 1) * chunk)
        cells = jnp.concatenate([held[0, part, :], held[1, part, :]], axis=1)
        term = jnp.dot(table[n % 2], cells, preferred_element_type=F32)
        if n == 0:
            total[...] = term
        else:
            total[...] += term
    rows = S // facets
    real = total[0:S, 0:W] + total[S : 2 * S, W : 2 * W]
    imag = total[0:S, W : 2 * W] - total[S : 2 * S, 0:W]
    total[0:S, 0:W] = real
    total[0:S, W : 2 * W] = imag
    extra = out.shape[2] - 2 * rows
    high = across >> 8
    low = across & 255
    note = jnp.where(
        lax.broadcasted_iota(I32, (extra, W), 0) == 0, high, low
    ).astype(F32).astype(BF16)
    for o in range(facets):
        re = total[o * rows : (o + 1) * rows, 0:W].astype(BF16)
        im = total[o * rows : (o + 1) * rows, W : 2 * W].astype(BF16)
        for c in range(cols):
            out[o, c, 0:rows, :] = re
            out[o, c, rows : 2 * rows, :] = im
            out[o, c, 2 * rows :, :] = note


def along(strip, scalars, facets, cols):
    count = strip.shape[1]
    chunk = min(1024, count)
    rows = S // facets
    return pl.pallas_call(
        functools.partial(along_kernel, facets, cols, chunk),
        out_shape=jax.ShapeDtypeStruct((facets, cols, 2 * rows + 8, W), BF16),
        in_specs=[
            pl.BlockSpec(memory_space=pltpu.SMEM),
            pl.BlockSpec(memory_space=pl.ANY),
        ],
        out_specs=pl.BlockSpec(memory_space=pltpu.VMEM),
        scratch_shapes=[
            pltpu.VMEM((2, count, W), BF16),
            pltpu.VMEM((2, 2 * S, chunk), BF16),
            pltpu.VMEM((2 * S, 2 * W), F32),
            pltpu.SemaphoreType.DMA((count // chunk,)),
        ],
        cost_estimate=pl.CostEstimate(
            flops=8 * S * W * count, bytes_accessed=4 * count * W, transcendentals=0
        ),
        name="along",
    )(scalars, strip)


def across_kernel(facets, cols, scal, got, out, left, summed):
    rows = S // facets
    column = scal[0]
    wide = 2 * S
    cell = lax.broadcasted_iota(I32, (W, wide), 0)
    lane = lax.broadcasted_iota(I32, (W, wide), 1)
    sample = (lane >> 6) * TILE + (lane & (TILE - 1))
    turn = ((lane >> 5) & 1) * (NTOT // 4)
    position = column + (NTOT // S) * sample
    top, bottom = cos_sin((cell * position + turn) & (NTOT - 1))
    scale = 1.0 / math.sqrt(W)
    right = jnp.concatenate([(top * scale).astype(BF16), (bottom * scale).astype(BF16)], axis=0)
    height = facets * rows
    for f in range(facets):
        re = got[f, 0, 0:rows, :].astype(F32)
        im = got[f, 0, rows : 2 * rows, :].astype(F32)
        for h in range(1, cols):
            re = re + got[f, h, 0:rows, :].astype(F32)
            im = im + got[f, h, rows : 2 * rows, :].astype(F32)
        left[f * rows : (f + 1) * rows, 0:W] = re
        left[f * rows : (f + 1) * rows, W : 2 * W] = im
        left[height + f * rows : height + (f + 1) * rows, 0:W] = im
        left[height + f * rows : height + (f + 1) * rows, W : 2 * W] = -re
    summed[...] = jnp.dot(left[...].astype(BF16), right, preferred_element_type=F32)
    acc = jnp.zeros((rows, wide), F32)
    for f in range(facets):
        note = got[f, 0, 2 * rows : 2 * rows + 8, :].astype(F32)
        offset = (note[0:1, 0:1] * 256.0 + note[1:2, 0:1]).astype(I32)
        cosine, sine = cos_sin(mod_phase(offset, position[0:1, :]))
        acc = acc + summed[f * rows : (f + 1) * rows, :] * cosine
        acc = acc + summed[height + f * rows : height + (f + 1) * rows, :] * sine
    acc = (acc * (1.0 / math.sqrt(facets))).astype(BF16)
    for o in range(facets):
        for m in range(wide // W):
            out[o, m] = acc[:, m * W : (m + 1) * W]


def across(got, scalars, facets, cols):
    rows = S // facets
    return pl.pallas_call(
        functools.partial(across_kernel, facets, cols),
        out_shape=jax.ShapeDtypeStruct((facets, 2 * S // W, rows, W), BF16),
        in_specs=[
            pl.BlockSpec(memory_space=pltpu.SMEM),
            pl.BlockSpec(memory_space=pltpu.VMEM),
        ],
        out_specs=pl.BlockSpec(memory_space=pltpu.VMEM),
        scratch_shapes=[
            pltpu.VMEM((2 * S, 2 * W), F32),
            pltpu.VMEM((2 * S, 2 * S), F32),
        ],
        cost_estimate=pl.CostEstimate(
            flops=2 * 2 * S * 2 * W * 2 * S, bytes_accessed=1 << 20, transcendentals=0
        ),
        name="across",
    )(scalars, got)


def visibility_kernel(facets, names, live, grid, uv, out, tile, right):
    rows = S // facets
    pieces = TILE // rows
    vis = uv.shape[2]
    step = NTOT // UV_STEPS
    sublane = lax.broadcasted_iota(I32, (TILE, vis), 0) * step
    lane = lax.broadcasted_iota(I32, (TILE, W), 1)
    sign = jnp.where((lane & TILE) == 0, 1.0, -1.0).astype(F32)

    def slot(j, carry):
        @pl.when(j < live[0])
        def _():
            name = names[j]
            a, b = name >> 3, name & 7
            for t in range(pieces):
                tile[t * rows : (t + 1) * rows, :] = grid[a * pieces + t, b >> 1].astype(F32)
            x = tile[...]
            y = pltpu.roll(x, 2 * TILE, 1)
            both = jnp.where((lane >= 2 * TILE) == ((b & 1) == 1), x, y)
            turned = pltpu.roll(both, TILE, 1)
            lhs = jnp.concatenate([both * sign, turned], axis=0).astype(BF16)
            cosine, sine = cos_sin((uv[j, 1:2, :] * sublane) & (NTOT - 1))
            cos_high, sin_high = cosine.astype(BF16), sine.astype(BF16)
            right[0:TILE, :] = cos_high
            right[TILE : 2 * TILE, :] = sin_high
            right[2 * TILE : 3 * TILE, :] = (cosine - cos_high.astype(F32)).astype(BF16)
            right[3 * TILE : 4 * TILE, :] = (sine - sin_high.astype(F32)).astype(BF16)
            middle = jnp.dot(lhs, right[...], preferred_element_type=F32)
            real, imag = middle[0:TILE], middle[TILE : 2 * TILE]
            cosine, sine = cos_sin((uv[j, 0:1, :] * sublane) & (NTOT - 1))
            scale = 1.0 / TILE
            out[j, 0:1, :] = jnp.sum(cosine * real - sine * imag, axis=0, keepdims=True) * scale
            out[j, 1:2, :] = jnp.sum(cosine * imag + sine * real, axis=0, keepdims=True) * scale

        @pl.when(j >= live[0])
        def _():
            out[j] = jnp.zeros((2, vis), F32)

        return carry

    lax.fori_loop(0, uv.shape[0], slot, 0)


def visibilities_of(grid, names, live, uv, facets):
    slots, _, vis = uv.shape
    return pl.pallas_call(
        functools.partial(visibility_kernel, facets),
        out_shape=jax.ShapeDtypeStruct((slots, 2, vis), F32),
        in_specs=[
            pl.BlockSpec(memory_space=pltpu.SMEM),
            pl.BlockSpec(memory_space=pltpu.SMEM),
            pl.BlockSpec(memory_space=pltpu.VMEM),
            pl.BlockSpec(memory_space=pltpu.VMEM),
        ],
        out_specs=pl.BlockSpec(memory_space=pltpu.VMEM),
        scratch_shapes=[
            pltpu.VMEM((TILE, W), F32),
            pltpu.VMEM((4 * TILE, vis), BF16),
        ],
        cost_estimate=pl.CostEstimate(
            flops=slots * 2 * 64 * 128 * vis, bytes_accessed=1 << 20, transcendentals=0
        ),
        name="visibility",
    )(names, live, grid, uv)


def shards(
    facet_strips, facet_offsets, column_offsets, row_offsets, tile_lists, tile_counts, uv_index
):
    facets, cols = lax.axis_size("facet"), lax.axis_size("col")
    strip = facet_strips[0]
    first_cell = lax.axis_index("col") * strip.shape[1]
    scalars = jnp.stack(
        [row_offsets[0], facet_offsets[0, 0] + first_cell, facet_offsets[0, 1]]
    ).astype(I32)
    sent = along(strip, scalars, facets, cols)
    flat = sent.reshape((facets * cols,) + sent.shape[2:])
    got = lax.all_to_all(flat, ("facet", "col"), 0, 0)
    owned = across(got.reshape(sent.shape), column_offsets, facets, cols)
    grid = lax.all_to_all(owned, "facet", 0, 0)
    result = visibilities_of(grid, tile_lists[0, 0], tile_counts[0], uv_index[0, 0], facets)
    return result[None, None]


def solution(mesh):
    in_specs = (
        P("facet", None, "col", None),
        P("facet", None),
        P("col"),
        P(),
        P("col", "facet", None),
        P("col", "facet"),
        P("col", "facet", None, None, None),
    )
    out_specs = P("col", "facet", None, None, None)
    return jax.shard_map(shards, mesh=mesh, in_specs=in_specs, out_specs=out_specs, check_vma=False)
```

```python
import functools
import math

import jax
import jax.numpy as jnp
from jax import lax
from jax.experimental import pallas as pl
from jax.experimental.pallas import tpu as pltpu
from jax.sharding import PartitionSpec as P


L = 8192
W = 128
S = 256
TILE = 32
NTOT = 65536
UV_STEPS = 4096
VMEM_LIMIT = 16 << 20
BF16 = jnp.bfloat16
F32 = jnp.float32
I32 = jnp.int32


def cos_sin(index):
    shifted = index + NTOT // 8
    quadrant = shifted >> 14
    rest = (shifted & (NTOT // 4 - 1)) - NTOT // 8
    x = rest.astype(F32) * (2.0 * math.pi / NTOT)
    y = x * x
    sine = x + x * (y * (-1.0 / 6 + y * (1.0 / 120 + y * (-1.0 / 5040 + y * (1.0 / 362880)))))
    cosine = 1.0 + y * (-0.5 + y * (1.0 / 24 + y * (-1.0 / 720 + y * (1.0 / 40320))))
    odd = (quadrant & 1) != 0
    first = jnp.where(odd, sine, cosine)
    second = jnp.where(odd, cosine, sine)
    return (
        jnp.where(((quadrant + 1) & 2) != 0, -first, first),
        jnp.where((quadrant & 2) != 0, -second, second),
    )


def mod_phase(first, second):
    return (first * second) & (NTOT - 1)


def along_kernel(chunk, rows_at, offsets, strip, rounded, own, held, table, total, sems):
    count = held.shape[1]
    steps = count // chunk
    copies = []
    for n in range(steps):
        part = pl.ds(n * chunk, chunk)
        copies.append(pltpu.make_async_copy(strip.at[:, part], held.at[:, part], sems.at[n]))
        copies[n].start()
    row_start = rows_at[0]
    col_start = offsets[0, 0] + lax.axis_index("col") * count
    row = row_start + (NTOT // L) * lax.broadcasted_iota(I32, (S, W), 0)
    lane = lax.broadcasted_iota(I32, (S, W), 1)
    cos_in, sin_in = cos_sin(mod_phase(row, lane))
    cos_out, sin_out = cos_sin(mod_phase(row, col_start + W * lane))
    scale = 1.0 / math.sqrt(L)
    cos_out = cos_out * scale
    sin_out = sin_out * scale
    for n in range(steps):
        for local in range(chunk // W):
            a = n * (chunk // W) + local
            c = cos_out[:, a : a + 1]
            s = sin_out[:, a : a + 1]
            place = slice(local * W, (local + 1) * W)
            table[n % 2, 0:S, place] = (c * cos_in - s * sin_in).astype(BF16)
            table[n % 2, S : 2 * S, place] = (s * cos_in + c * sin_in).astype(BF16)
        copies[n].wait()
        part = slice(n * chunk, (n + 1) * chunk)
        cells = jnp.concatenate([held[0, part, :], held[1, part, :]], axis=1)
        term = jnp.dot(table[n % 2], cells, preferred_element_type=F32)
        if n == 0:
            total[...] = term
        else:
            total[...] += term
    real = total[0:S, 0:W] + total[S : 2 * S, W : 2 * W]
    imag = total[0:S, W : 2 * W] - total[S : 2 * S, 0:W]
    own[:, 0:W] = real
    own[:, W : 2 * W] = imag
    rounded[:, 0:W] = real.astype(BF16)
    rounded[:, W : 2 * W] = imag.astype(BF16)


def along(strip, row_offsets, facet_offsets):
    count = strip.shape[1]
    chunk = min(1024, count)
    return pl.pallas_call(
        functools.partial(along_kernel, chunk),
        out_shape=(
            jax.ShapeDtypeStruct((S, 2 * W), BF16),
            jax.ShapeDtypeStruct((S, 2 * W), F32),
        ),
        in_specs=[
            pl.BlockSpec(memory_space=pltpu.SMEM),
            pl.BlockSpec(memory_space=pltpu.SMEM),
            pl.BlockSpec(memory_space=pltpu.HBM),
        ],
        out_specs=[pl.BlockSpec(memory_space=pltpu.VMEM)] * 2,
        scratch_shapes=[
            pltpu.VMEM((2, count, W), BF16),
            pltpu.VMEM((2, 2 * S, chunk), BF16),
            pltpu.VMEM((2 * S, 2 * W), F32),
            pltpu.SemaphoreType.DMA((count // chunk,)),
        ],
        compiler_params=pltpu.CompilerParams(vmem_limit_bytes=VMEM_LIMIT),
        cost_estimate=pl.CostEstimate(
            flops=8 * S * W * count, bytes_accessed=4 * count * W, transcendentals=0
        ),
        name="along",
    )(row_offsets, facet_offsets, strip)


def across_kernel(columns, offsets, names, own, other, keep, send, terms):
    facets, slots = names.shape[0], names.shape[2]
    wide = 2 * S
    cell = lax.broadcasted_iota(I32, (W, wide), 0)
    lane = lax.broadcasted_iota(I32, (W, wide), 1)
    sample = (lane >> 6) * TILE + (lane & (TILE - 1))
    turn = ((lane >> 5) & 1) * (NTOT // 4)
    position = columns[0] + (NTOT // S) * sample
    top, bottom = cos_sin(((offsets[0, 1] + cell) * position + turn) & (NTOT - 1))
    scale = 1.0 / math.sqrt(W)
    right = jnp.concatenate([(top * scale).astype(BF16), (bottom * scale).astype(BF16)], axis=0)
    strip_rows = own[...]
    if other is not None:
        strip_rows = strip_rows + other[...].astype(F32)
    product = jnp.dot(strip_rows.astype(BF16), right, preferred_element_type=F32)
    for a in range(S // TILE):
        for m in range(wide // W):
            block = product[a * TILE : (a + 1) * TILE, m * W : (m + 1) * W]
            terms[0, a, m] = block
            terms[1, a, m] = pltpu.roll(block, W // 2, 1)
    core = lax.axis_index("facet") & 1
    first_half = lax.broadcasted_iota(I32, (TILE, W), 1) < W // 2

    def pair(o, slot):
        even, odd = names[o, 0, slot], names[o, 0, slot + 1]
        return jnp.where(
            first_half,
            terms[even & 1, even >> 3, (even & 7) >> 1],
            terms[1 - (odd & 1), odd >> 3, (odd & 7) >> 1],
        )

    def owner(o, carry):
        for n in range(slots // 4):
            keep[o, n] = pair(o, core * (slots // 2) + 2 * n)
            send[o, n] = pair(o, (1 - core) * (slots // 2) + 2 * n).astype(BF16)
        return carry

    lax.fori_loop(0, facets, owner, 0, unroll=4)


def across(own, other, columns, offsets, names):
    facets, _, slots = names.shape
    shape = (facets, slots // 4, TILE, W)
    kernel = across_kernel
    arrays = [own]
    if other is None:
        kernel = lambda c, f, n, own, *rest: across_kernel(c, f, n, own, None, *rest)
    else:
        arrays.append(other)
    return pl.pallas_call(
        kernel,
        out_shape=(jax.ShapeDtypeStruct(shape, F32), jax.ShapeDtypeStruct(shape, BF16)),
        in_specs=[pl.BlockSpec(memory_space=pltpu.SMEM)] * 3
        + [pl.BlockSpec(memory_space=pltpu.VMEM)] * len(arrays),
        out_specs=[pl.BlockSpec(memory_space=pltpu.VMEM)] * 2,
        scratch_shapes=[pltpu.VMEM((2, S // TILE, 2 * S // W, TILE, W), F32)],
        compiler_params=pltpu.CompilerParams(vmem_limit_bytes=VMEM_LIMIT),
        cost_estimate=pl.CostEstimate(
            flops=2 * S * 2 * W * 2 * S, bytes_accessed=1 << 20, transcendentals=0
        ),
        name="across",
    )(columns, offsets, names, *arrays)


def visibility_kernel(live, parts, uv, out, tiles, right):
    facets, pairs = parts.shape[0], parts.shape[1]
    vis = uv.shape[2]
    step = NTOT // UV_STEPS
    sublane = lax.broadcasted_iota(I32, (TILE, vis), 0) * step
    lane = lax.broadcasted_iota(I32, (TILE, W), 1)
    sign = jnp.where((lane & TILE) == 0, 1.0, -1.0).astype(F32)
    scale = 1.0 / math.sqrt(facets)
    for core in range(2):
        for n in range(pairs):
            acc = parts[core, n].astype(F32)
            for f in range(core + 2, facets, 2):
                acc = acc + parts[f, n].astype(F32)
            acc = (acc * scale).astype(BF16).astype(F32)
            turned = pltpu.roll(acc, W // 2, 1)
            tiles[core * 2 * pairs + 2 * n] = jnp.where(lane < W // 2, acc, turned)
            tiles[core * 2 * pairs + 2 * n + 1] = jnp.where(lane < W // 2, turned, acc)

    def slot(j, carry):
        @pl.when(j < live[0, 0])
        def _():
            both = tiles[j]
            turned = pltpu.roll(both, TILE, 1)
            lhs = jnp.concatenate([both * sign, turned], axis=0).astype(BF16)
            cosine, sine = cos_sin((uv[j, 1:2, :] * sublane) & (NTOT - 1))
            cos_high, sin_high = cosine.astype(BF16), sine.astype(BF16)
            right[0:TILE, :] = cos_high
            right[TILE : 2 * TILE, :] = sin_high
            right[2 * TILE : 3 * TILE, :] = (cosine - cos_high.astype(F32)).astype(BF16)
            right[3 * TILE : 4 * TILE, :] = (sine - sin_high.astype(F32)).astype(BF16)
            middle = jnp.dot(lhs, right[...], preferred_element_type=F32)
            real, imag = middle[0:TILE], middle[TILE : 2 * TILE]
            cosine, sine = cos_sin((uv[j, 0:1, :] * sublane) & (NTOT - 1))
            size = 1.0 / TILE
            out[j, 0:1, :] = jnp.sum(cosine * real - sine * imag, axis=0, keepdims=True) * size
            out[j, 1:2, :] = jnp.sum(cosine * imag + sine * real, axis=0, keepdims=True) * size

        @pl.when(j >= live[0, 0])
        def _():
            out[j] = jnp.zeros((2, vis), F32)

        return carry

    lax.fori_loop(0, uv.shape[0], slot, 0)


def visibilities_of(parts, live, uv):
    slots, _, vis = uv.shape
    return pl.pallas_call(
        visibility_kernel,
        out_shape=jax.ShapeDtypeStruct((slots, 2, vis), F32),
        in_specs=[
            pl.BlockSpec(memory_space=pltpu.SMEM),
            pl.BlockSpec(memory_space=pltpu.VMEM),
            pl.BlockSpec(memory_space=pltpu.VMEM),
        ],
        out_specs=pl.BlockSpec(memory_space=pltpu.VMEM),
        scratch_shapes=[
            pltpu.VMEM((slots, TILE, W), F32),
            pltpu.VMEM((4 * TILE, vis), BF16),
        ],
        compiler_params=pltpu.CompilerParams(vmem_limit_bytes=VMEM_LIMIT),
        cost_estimate=pl.CostEstimate(
            flops=slots * 2 * 64 * 128 * vis, bytes_accessed=1 << 20, transcendentals=0
        ),
        name="visibility",
    )(live, parts, uv)


def shards(
    facet_strips, facet_offsets, column_offsets, row_offsets, tile_lists, tile_counts, uv_index
):
    facets, cols = lax.axis_size("facet"), lax.axis_size("col")
    slots = tile_lists.shape[2]
    names = lax.all_to_all(
        jnp.broadcast_to(tile_lists, (facets, 1, slots)), "facet", 0, 0, tiled=True
    )
    rounded, own = along(facet_strips[0], row_offsets, facet_offsets)
    other = None
    if cols == 2:
        other = lax.ppermute(rounded, "col", [(0, 1), (1, 0)])
    else:
        own = lax.psum(own, "col")
    keep, send = across(own, other, column_offsets, facet_offsets, names)
    swapped = lax.ppermute(send, "facet", [(f, f ^ 1) for f in range(facets)])
    both = (keep + swapped.astype(F32)).astype(BF16)
    parts = lax.all_to_all(both, "facet", 0, 0, tiled=True)
    result = visibilities_of(parts, tile_counts, uv_index[0, 0])
    return result[None, None]


def solution(mesh):
    in_specs = (
        P("facet", None, "col", None),
        P("facet", None),
        P("col"),
        P(),
        P("col", "facet", None),
        P("col", "facet"),
        P("col", "facet", None, None, None),
    )
    out_specs = P("col", "facet", None, None, None)
    return jax.shard_map(shards, mesh=mesh, in_specs=in_specs, out_specs=out_specs, check_vma=False)
```

```python
import functools
import math

import jax
import jax.numpy as jnp
from jax import lax
from jax.experimental import pallas as pl
from jax.experimental.pallas import tpu as pltpu
from jax.sharding import PartitionSpec as P


L = 8192
W = 128
S = 256
TILE = 32
NTOT = 65536
UV_STEPS = 4096
VMEM_LIMIT = 16 << 20
BF16 = jnp.bfloat16
F32 = jnp.float32
I32 = jnp.int32


def cos_sin(index):
    shifted = index + NTOT // 8
    quadrant = shifted >> 14
    rest = (shifted & (NTOT // 4 - 1)) - NTOT // 8
    x = rest.astype(F32) * (2.0 * math.pi / NTOT)
    y = x * x
    sine = x + x * (y * (-1.0 / 6 + y * (1.0 / 120 + y * (-1.0 / 5040 + y * (1.0 / 362880)))))
    cosine = 1.0 + y * (-0.5 + y * (1.0 / 24 + y * (-1.0 / 720 + y * (1.0 / 40320))))
    odd = (quadrant & 1) != 0
    first = jnp.where(odd, sine, cosine)
    second = jnp.where(odd, cosine, sine)
    return (
        jnp.where(((quadrant + 1) & 2) != 0, -first, first),
        jnp.where((quadrant & 2) != 0, -second, second),
    )


def mod_phase(first, second):
    return (first * second) & (NTOT - 1)


def split(facets):
    groups = max(1, facets // TILE)
    inside = TILE * groups // facets
    return groups, S // TILE // groups, inside


def along_kernel(facets, cols, chunk, scal, offsets, names, strip, out, held, table, total, small, sems):
    count = held.shape[1]
    steps = count // chunk
    slots = names.shape[2]
    copies = []
    notes = []
    for n, (src, dst) in enumerate(zip((offsets, names), small)):
        notes.append(pltpu.make_async_copy(src, dst, sems.at[steps + n]))
        notes[n].start()
    for n in range(steps):
        part = pl.ds(n * chunk, chunk)
        copies.append(pltpu.make_async_copy(strip.at[:, part], held.at[:, part], sems.at[n]))
        copies[n].start()
    for copy in notes:
        copy.wait()
    row_start = scal[0]
    col_start = small[0][0, 0] + lax.axis_index("col") * count
    rows = S // facets
    groups, tall, inside = split(facets)
    place = lax.broadcasted_iota(I32, (S, W), 0)
    lane = lax.broadcasted_iota(I32, (S, W), 1)
    owner = place // rows
    within = place % rows
    sample = (
        (within % tall + tall * (owner // (facets // groups))) * TILE
        + (owner % (facets // groups)) * inside
        + within // tall
    )
    row = row_start + (NTOT // L) * sample
    cos_in, sin_in = cos_sin(mod_phase(row, lane))
    cos_out, sin_out = cos_sin(mod_phase(row, col_start + W * lane))
    scale = 1.0 / math.sqrt(L)
    cos_out = cos_out * scale
    sin_out = sin_out * scale
    for n in range(steps):
        for local in range(chunk // W):
            a = n * (chunk // W) + local
            c = cos_out[:, a : a + 1]
            s = sin_out[:, a : a + 1]
            at = slice(local * W, (local + 1) * W)
            table[n % 2, 0:S, at] = (c * cos_in - s * sin_in).astype(BF16)
            table[n % 2, S : 2 * S, at] = (s * cos_in + c * sin_in).astype(BF16)
        copies[n].wait()
        part = slice(n * chunk, (n + 1) * chunk)
        cells = jnp.concatenate([held[0, part, :], held[1, part, :]], axis=1)
        term = jnp.dot(table[n % 2], cells, preferred_element_type=F32)
        if n == 0:
            total[...] = term
        else:
            total[...] += term
    real = total[0:S, 0:W] + total[S : 2 * S, W : 2 * W]
    imag = total[0:S, W : 2 * W] - total[S : 2 * S, 0:W]
    total[0:S, 0:W] = real
    total[0:S, W : 2 * W] = imag
    across = small[0][0, 1]
    line = lax.broadcasted_iota(I32, (slots, W), 0)
    spot = lax.broadcasted_iota(I32, (slots, W), 1)
    note = jnp.zeros((slots, W), I32)
    for j in range(slots):
        note = jnp.where(line == j, small[1][0, 0, j], note)
    note = jnp.where(spot == W - 2, across >> 8, jnp.where(spot == W - 1, across & 255, note))
    note = note.astype(F32).astype(BF16)
    for o in range(facets):
        re = total[o * rows : (o + 1) * rows, 0:W].astype(BF16)
        im = total[o * rows : (o + 1) * rows, W : 2 * W].astype(BF16)
        for c in range(cols):
            out[o * cols + c, 0:rows, :] = re
            out[o * cols + c, rows : 2 * rows, :] = im
            out[o * cols + c, 2 * rows :, :] = note


def along(strip, row_offsets, facet_offsets, names, facets, cols):
    count = strip.shape[1]
    chunk = min(1024, count)
    rows = S // facets
    slots = names.shape[2]
    return pl.pallas_call(
        functools.partial(along_kernel, facets, cols, chunk),
        out_shape=jax.ShapeDtypeStruct((facets * cols, 2 * rows + slots, W), BF16),
        in_specs=[pl.BlockSpec(memory_space=pltpu.SMEM)]
        + [pl.BlockSpec(memory_space=pltpu.HBM)] * 3,
        out_specs=pl.BlockSpec(memory_space=pltpu.VMEM),
        scratch_shapes=[
            pltpu.VMEM((2, count, W), BF16),
            pltpu.VMEM((2, 2 * S, chunk), BF16),
            pltpu.VMEM((2 * S, 2 * W), F32),
            [
                pltpu.SMEM(facet_offsets.shape, I32),
                pltpu.SMEM(names.shape, I32),
            ],
            pltpu.SemaphoreType.DMA((count // chunk + 2,)),
        ],
        cost_estimate=pl.CostEstimate(
            flops=8 * S * W * count, bytes_accessed=4 * count * W, transcendentals=0
        ),
        name="along",
    )(row_offsets, facet_offsets, names, strip)


def base_kernel(columns, out):
    cell = lax.broadcasted_iota(I32, (W, 2 * S), 0)
    lane = lax.broadcasted_iota(I32, (W, 2 * S), 1)
    turn = ((lane >> 5) & 1) * (NTOT // 4)
    top, bottom = cos_sin((cell * positions(columns[0], lane) + turn) & (NTOT - 1))
    scale = 1.0 / math.sqrt(W)
    out[0:W, :] = (top * scale).astype(BF16)
    out[W : 2 * W, :] = (bottom * scale).astype(BF16)


def positions(column, lane):
    return column + (NTOT // S) * ((lane >> 6) * TILE + (lane & (TILE - 1)))


def base(columns):
    return pl.pallas_call(
        base_kernel,
        out_shape=jax.ShapeDtypeStruct((2 * W, 2 * S), BF16),
        in_specs=[pl.BlockSpec(memory_space=pltpu.SMEM)],
        out_specs=pl.BlockSpec(memory_space=pltpu.VMEM),
        compiler_params=pltpu.CompilerParams(vmem_limit_bytes=VMEM_LIMIT),
        cost_estimate=pl.CostEstimate(flops=1 << 24, bytes_accessed=1 << 18, transcendentals=0),
        name="base",
    )(columns)


def across_kernel(facets, cols, columns, got, right, out, left, summed, phases):
    rows = S // facets
    groups, tall, inside = split(facets)
    slots = got.shape[1] - 2 * rows
    wide = 2 * S
    height = facets * rows
    column = lax.axis_index("col")
    sources = []
    for f in range(facets):
        re = got[f * cols, 0:rows, :].astype(F32)
        im = got[f * cols, rows : 2 * rows, :].astype(F32)
        for h in range(1, cols):
            re = re + got[f * cols + h, 0:rows, :].astype(F32)
            im = im + got[f * cols + h, rows : 2 * rows, :].astype(F32)
        left[f * rows : (f + 1) * rows, 0:W] = re
        left[f * rows : (f + 1) * rows, W : 2 * W] = im
        left[height + f * rows : height + (f + 1) * rows, 0:W] = im
        left[height + f * rows : height + (f + 1) * rows, W : 2 * W] = -re
        sources.append(got[f * cols + column, 2 * rows :, :].astype(F32))
    summed[...] = jnp.dot(left[...].astype(BF16), right[...], preferred_element_type=F32)
    heads = jnp.concatenate([note[0:1] for note in sources], axis=0)
    offset = (heads[:, W - 2 : W - 1] * 256.0 + heads[:, W - 1 : W]).astype(I32)
    lane = lax.broadcasted_iota(I32, (facets, wide), 1)
    cosine, sine = cos_sin(mod_phase(offset, positions(columns[0], lane)))
    phases[0] = cosine
    phases[1] = sine
    acc = jnp.zeros((rows, wide), F32)
    for f in range(facets):
        acc = acc + summed[f * rows : (f + 1) * rows, :] * phases[0, f : f + 1, :]
        acc = acc + summed[height + f * rows : height + (f + 1) * rows, :] * phases[1, f : f + 1, :]
    acc = acc * (1.0 / math.sqrt(facets))
    pieces = []
    for b in range(S // TILE):
        at = slice(b * 2 * TILE, (b + 1) * 2 * TILE)
        parts = [acc[i * tall : (i + 1) * tall, at] for i in range(inside)]
        if inside == 1:
            parts.append(jnp.zeros_like(parts[0]))
        pieces.append(jnp.concatenate(parts, axis=1))
    tiles = jnp.concatenate(pieces, axis=0).astype(BF16)
    names = jnp.concatenate(sources, axis=0).astype(I32)
    first = (lax.axis_index("facet") // (facets // groups)) * tall
    local = (names >> 3) - first
    wanted = jnp.where((local >= 0) & (local < tall), (names & 7) * tall + local, -1)
    count = tiles.shape[0]
    spot = lax.broadcasted_iota(I32, (facets * slots, W), 1)
    onehot = jnp.where(wanted == spot, 1.0, 0.0).astype(BF16)[:, 0:count]
    chosen = jnp.dot(onehot, tiles, preferred_element_type=F32)
    for o in range(facets):
        out[o] = chosen[o * slots : (o + 1) * slots, :].astype(BF16)


def across(got, right, columns, facets, cols):
    rows = S // facets
    slots = got.shape[1] - 2 * rows
    return pl.pallas_call(
        functools.partial(across_kernel, facets, cols),
        out_shape=jax.ShapeDtypeStruct((facets, slots, W), BF16),
        in_specs=[
            pl.BlockSpec(memory_space=pltpu.SMEM),
            pl.BlockSpec(memory_space=pltpu.VMEM),
            pl.BlockSpec(memory_space=pltpu.VMEM),
        ],
        out_specs=pl.BlockSpec(memory_space=pltpu.VMEM),
        scratch_shapes=[
            pltpu.VMEM((2 * S, 2 * W), F32),
            pltpu.VMEM((2 * S, 2 * S), F32),
            pltpu.VMEM((2, facets, 2 * S), F32),
        ],
        compiler_params=pltpu.CompilerParams(vmem_limit_bytes=VMEM_LIMIT),
        cost_estimate=pl.CostEstimate(
            flops=2 * 2 * S * 2 * W * 2 * S, bytes_accessed=1 << 20, transcendentals=0
        ),
        name="across",
    )(columns, got, right)


def waves_kernel(facets, uv, right, near, far):
    _, _, inside = split(facets)
    vis = uv.shape[2]
    step = NTOT // UV_STEPS
    line = lax.broadcasted_iota(I32, (TILE, vis), 0)
    low = line[0:8] * inside
    high = (line[0:4] % (4 // inside)) * 8 * inside + line[0:4] // (4 // inside)

    def slot(j, carry):
        cosine, sine = cos_sin((uv[j, 1:2, :] * (line * step)) & (NTOT - 1))
        cos_high, sin_high = cosine.astype(BF16), sine.astype(BF16)
        right[j, 0:TILE, :] = cos_high
        right[j, TILE : 2 * TILE, :] = sin_high
        right[j, 2 * TILE : 3 * TILE, :] = (cosine - cos_high.astype(F32)).astype(BF16)
        right[j, 3 * TILE : 4 * TILE, :] = (sine - sin_high.astype(F32)).astype(BF16)
        cosine, sine = cos_sin((uv[j, 0:1, :] * (low * step)) & (NTOT - 1))
        near[j, 0] = cosine * (1.0 / TILE)
        near[j, 1] = sine * (1.0 / TILE)
        cosine, sine = cos_sin((uv[j, 0:1, :] * (high * step)) & (NTOT - 1))
        far[j, 0] = cosine
        far[j, 1] = sine
        return carry

    lax.fori_loop(0, uv.shape[0], slot, 0)


def waves(uv, facets):
    slots, _, vis = uv.shape
    return pl.pallas_call(
        functools.partial(waves_kernel, facets),
        out_shape=(
            jax.ShapeDtypeStruct((slots, 4 * TILE, vis), BF16),
            jax.ShapeDtypeStruct((slots, 2, 8, vis), F32),
            jax.ShapeDtypeStruct((slots, 2, 4, vis), F32),
        ),
        in_specs=[pl.BlockSpec(memory_space=pltpu.VMEM)],
        out_specs=[pl.BlockSpec(memory_space=pltpu.VMEM)] * 3,
        compiler_params=pltpu.CompilerParams(vmem_limit_bytes=VMEM_LIMIT),
        cost_estimate=pl.CostEstimate(flops=1 << 26, bytes_accessed=3 << 20, transcendentals=0),
        name="waves",
    )(uv)


def visibility_kernel(facets, live, parts, right, near, far, out, held):
    groups, _, inside = split(facets)
    slots, vis = out.shape[0], out.shape[2]
    sources = facets // groups
    for f in range(sources):
        held[f] = parts[f].astype(F32)
        for g in range(1, groups):
            held[f] += parts[g * sources + f].astype(F32)
    lane = lax.broadcasted_iota(I32, (sources, W), 1)
    sign = jnp.where((lane & TILE) == 0, 1.0, -1.0).astype(F32)
    for j in range(slots):
        @pl.when(j < live[0, 0])
        def _():
            x = held[:, j, :]
            y = pltpu.roll(x, W // 2, 1)
            both = [jnp.where(lane < W // 2, x, y), jnp.where(lane < W // 2, y, x)][:inside]
            lhs = [z * sign for z in both] + [pltpu.roll(z, TILE, 1) for z in both]
            middle = jnp.dot(
                jnp.concatenate(lhs, axis=0).astype(BF16), right[j], preferred_element_type=F32
            )
            real, imag = middle[0:8], middle[TILE : TILE + 8]
            for h in range(1, 4):
                more_re = middle[8 * h : 8 * h + 8]
                more_im = middle[TILE + 8 * h : TILE + 8 * h + 8]
                cosine, sine = far[j, 0, h : h + 1, :], far[j, 1, h : h + 1, :]
                real = real + (cosine * more_re - sine * more_im)
                imag = imag + (cosine * more_im + sine * more_re)
            cosine, sine = near[j, 0], near[j, 1]
            out[j, 0:1, :] = jnp.sum(cosine * real - sine * imag, axis=0, keepdims=True)
            out[j, 1:2, :] = jnp.sum(cosine * imag + sine * real, axis=0, keepdims=True)

        @pl.when(j >= live[0, 0])
        def _():
            out[j] = jnp.zeros((2, vis), F32)


def visibilities_of(parts, live, tables, facets):
    slots, _, vis = tables[0].shape
    return pl.pallas_call(
        functools.partial(visibility_kernel, facets),
        out_shape=jax.ShapeDtypeStruct((slots, 2, vis), F32),
        in_specs=[pl.BlockSpec(memory_space=pltpu.SMEM)]
        + [pl.BlockSpec(memory_space=pltpu.VMEM)] * 4,
        out_specs=pl.BlockSpec(memory_space=pltpu.VMEM),
        scratch_shapes=[pltpu.VMEM((facets // split(facets)[0], slots, W), F32)],
        compiler_params=pltpu.CompilerParams(vmem_limit_bytes=VMEM_LIMIT),
        cost_estimate=pl.CostEstimate(
            flops=slots * 2 * 64 * 128 * vis, bytes_accessed=1 << 20, transcendentals=0
        ),
        name="visibility",
    )(live, parts, *tables)


def shards(
    facet_strips, facet_offsets, column_offsets, row_offsets, tile_lists, tile_counts, uv_index
):
    facets, cols = lax.axis_size("facet"), lax.axis_size("col")
    sent = along(facet_strips[0], row_offsets, facet_offsets, tile_lists, facets, cols)
    got = lax.all_to_all(sent, ("facet", "col"), 0, 0, tiled=True)
    right = base(column_offsets)
    asked = across(got, right, column_offsets, facets, cols)
    parts = lax.all_to_all(asked, "facet", 0, 0, tiled=True)
    tables = waves(uv_index[0, 0], facets)
    result = visibilities_of(parts, tile_counts, tables, facets)
    return result[None, None]


def solution(mesh):
    in_specs = (
        P("facet", None, "col", None),
        P("facet", None),
        P("col"),
        P(),
        P("col", "facet", None),
        P("col", "facet"),
        P("col", "facet", None, None, None),
    )
    out_specs = P("col", "facet", None, None, None)
    return jax.shard_map(shards, mesh=mesh, in_specs=in_specs, out_specs=out_specs, check_vma=False)
```

```python
import functools
import math

import jax
import jax.numpy as jnp
from jax import lax
from jax.experimental import pallas as pl
from jax.experimental.pallas import tpu as pltpu
from jax.sharding import PartitionSpec as P


L = 8192
W = 128
S = 256
TILE = 32
NTOT = 65536
UV_STEPS = 4096
VMEM_LIMIT = 16 << 20
CHUNK = 512
CHAIN = 16
BF16 = jnp.bfloat16
F32 = jnp.float32
I32 = jnp.int32


def cos_sin(index):
    shifted = index + NTOT // 8
    quadrant = shifted >> 14
    rest = (shifted & (NTOT // 4 - 1)) - NTOT // 8
    x = rest.astype(F32) * (2.0 * math.pi / NTOT)
    y = x * x
    sine = x + x * (y * (-1.0 / 6 + y * (1.0 / 120 + y * (-1.0 / 5040 + y * (1.0 / 362880)))))
    cosine = 1.0 + y * (-0.5 + y * (1.0 / 24 + y * (-1.0 / 720 + y * (1.0 / 40320))))
    odd = (quadrant & 1) != 0
    first = jnp.where(odd, sine, cosine)
    second = jnp.where(odd, cosine, sine)
    return (
        jnp.where(((quadrant + 1) & 2) != 0, -first, first),
        jnp.where((quadrant & 2) != 0, -second, second),
    )


def mod_phase(first, second):
    return (first * second) & (NTOT - 1)


def split(facets):
    groups = max(1, facets // TILE)
    inside = TILE * groups // facets
    return groups, S // TILE // groups, inside


def along_kernel(facets, cols, chunk, scal, offsets, names, strip, out, held, table, total, state, outside, small, sems):
    count = held.shape[1]
    steps = count // chunk
    slots = names.shape[2]
    copies = []
    notes = []
    for n, (src, dst) in enumerate(zip((offsets, names), small)):
        notes.append(pltpu.make_async_copy(src, dst, sems.at[steps + n]))
        notes[n].start()
    for n in range(steps):
        part = pl.ds(n * chunk, chunk)
        copies.append(pltpu.make_async_copy(strip.at[:, part], held.at[:, part], sems.at[n]))
        copies[n].start()
    for copy in notes:
        copy.wait()
    row_start = scal[0]
    col_start = small[0][0, 0] + lax.axis_index("col") * count
    rows = S // facets
    groups, tall, inside = split(facets)

    def sample_of(place):
        owner = place // rows
        within = place % rows
        group = owner // (facets // groups)
        line = (owner % (facets // groups)) * inside + within // tall
        return (within % tall + tall * group) * TILE + line

    blocks = S // 8
    inner = row_start + (NTOT // L) * sample_of(lax.broadcasted_iota(I32, (8, W), 0))
    outer = (NTOT // L) * sample_of(8 * lax.broadcasted_iota(I32, (blocks, W), 0))
    cell = col_start + lax.broadcasted_iota(I32, (8, W), 1)
    cells_of = {"first": (cell, 1.0 / math.sqrt(L)), "step": (W, 1.0), "leap": (CHAIN * W, 1.0)}
    factors = []
    for n, (column, scale) in enumerate(cells_of.values()):
        cosine, sine = cos_sin(mod_phase(inner, column))
        factors.append((cosine * scale, sine * scale))
        if n == 0:
            column = col_start + lax.broadcasted_iota(I32, (blocks, W), 1)
        cosine, sine = cos_sin(mod_phase(outer, column))
        outside[2 * n] = cosine
        outside[2 * n + 1] = sine

    def factor(n, k):
        cosine, sine = outside[2 * n, k : k + 1, :], outside[2 * n + 1, k : k + 1, :]
        x, y = factors[n]
        return x * cosine - y * sine, y * cosine + x * sine

    def fill(n):
        slot = n % 2
        for k in range(blocks):
            at = slice(8 * k, 8 * k + 8)
            twice = None
            for local in range(chunk // W):
                stage = (n * (chunk // W) + local) % CHAIN
                if stage == 0:
                    if n == 0:
                        c1, s1 = factor(0, k)
                    else:
                        leap_c, leap_s = factor(2, k)
                        c0, s0 = state[4, at], state[5, at]
                        c1, s1 = c0 * leap_c - s0 * leap_s, s0 * leap_c + c0 * leap_s
                    if (n + 1) * chunk < count:
                        state[4, at], state[5, at] = c1, s1
                elif stage == 1:
                    turn_c, turn_s = factor(1, k)
                    twice = turn_c + turn_c
                    state[6, at] = twice
                    c0, s0 = c1, s1
                    c1, s1 = c0 * turn_c - s0 * turn_s, s0 * turn_c + c0 * turn_s
                else:
                    if twice is None:
                        twice = state[6, at]
                        c0, s0, c1, s1 = (state[i, at] for i in range(4))
                    c0, c1 = c1, twice * c1 - c0
                    s0, s1 = s1, twice * s1 - s0
                place = slice(local * W, (local + 1) * W)
                table[slot, at, place] = c1.astype(BF16)
                table[slot, S + 8 * k : S + 8 * k + 8, place] = s1.astype(BF16)
            if (n + 1) * (chunk // W) % CHAIN:
                for i, value in enumerate((c0, s0, c1, s1)):
                    state[i, at] = value

    fill(0)
    for n in range(steps):
        copies[n].wait()
        if n + 1 < steps:
            fill(n + 1)
        part = slice(n * chunk, (n + 1) * chunk)
        cells = jnp.concatenate([held[0, part, :], held[1, part, :]], axis=1)
        term = jnp.dot(table[n % 2], cells, preferred_element_type=F32)
        if n == 0:
            total[...] = term
        else:
            total[...] += term
    real = total[0:S, 0:W] + total[S : 2 * S, W : 2 * W]
    imag = total[0:S, W : 2 * W] - total[S : 2 * S, 0:W]
    total[0:S, 0:W] = real
    total[0:S, W : 2 * W] = imag
    across = small[0][0, 1]
    line = lax.broadcasted_iota(I32, (slots, W), 0)
    spot = lax.broadcasted_iota(I32, (slots, W), 1)
    note = jnp.zeros((slots, W), I32)
    for j in range(slots):
        note = jnp.where(line == j, small[1][0, 0, j], note)
    note = jnp.where(spot == W - 2, across >> 8, jnp.where(spot == W - 1, across & 255, note))
    note = note.astype(F32).astype(BF16)
    for o in range(facets):
        re = total[o * rows : (o + 1) * rows, 0:W].astype(BF16)
        im = total[o * rows : (o + 1) * rows, W : 2 * W].astype(BF16)
        for c in range(cols):
            out[o * cols + c, 0:rows, :] = re
            out[o * cols + c, rows : 2 * rows, :] = im
            out[o * cols + c, 2 * rows :, :] = note


def along(strip, row_offsets, facet_offsets, names, facets, cols):
    count = strip.shape[1]
    chunk = min(CHUNK, count)
    rows = S // facets
    slots = names.shape[2]
    return pl.pallas_call(
        functools.partial(along_kernel, facets, cols, chunk),
        out_shape=jax.ShapeDtypeStruct((facets * cols, 2 * rows + slots, W), BF16),
        in_specs=[pl.BlockSpec(memory_space=pltpu.SMEM)]
        + [pl.BlockSpec(memory_space=pltpu.HBM)] * 3,
        out_specs=pl.BlockSpec(memory_space=pltpu.VMEM),
        scratch_shapes=[
            pltpu.VMEM((2, count, W), BF16),
            pltpu.VMEM((2, 2 * S, chunk), BF16),
            pltpu.VMEM((2 * S, 2 * W), F32),
            pltpu.VMEM((7, S, W), F32),
            pltpu.VMEM((6, S // 8, W), F32),
            [
                pltpu.SMEM(facet_offsets.shape, I32),
                pltpu.SMEM(names.shape, I32),
            ],
            pltpu.SemaphoreType.DMA((count // chunk + 2,)),
        ],
        cost_estimate=pl.CostEstimate(
            flops=8 * S * W * count, bytes_accessed=4 * count * W, transcendentals=0
        ),
        name="along",
    )(row_offsets, facet_offsets, names, strip)


def base_kernel(columns, out):
    cell = lax.broadcasted_iota(I32, (W, 2 * S), 0)
    lane = lax.broadcasted_iota(I32, (W, 2 * S), 1)
    turn = ((lane >> 5) & 1) * (NTOT // 4)
    top, bottom = cos_sin((cell * positions(columns[0], lane) + turn) & (NTOT - 1))
    scale = 1.0 / math.sqrt(W)
    out[0:W, :] = (top * scale).astype(BF16)
    out[W : 2 * W, :] = (bottom * scale).astype(BF16)


def positions(column, lane):
    return column + (NTOT // S) * ((lane >> 6) * TILE + (lane & (TILE - 1)))


def base(columns):
    return pl.pallas_call(
        base_kernel,
        out_shape=jax.ShapeDtypeStruct((2 * W, 2 * S), BF16),
        in_specs=[pl.BlockSpec(memory_space=pltpu.SMEM)],
        out_specs=pl.BlockSpec(memory_space=pltpu.VMEM),
        compiler_params=pltpu.CompilerParams(vmem_limit_bytes=VMEM_LIMIT),
        cost_estimate=pl.CostEstimate(flops=1 << 24, bytes_accessed=1 << 18, transcendentals=0),
        name="base",
    )(columns)


def across_kernel(facets, cols, columns, got, right, out, left, summed, phases):
    rows = S // facets
    groups, tall, inside = split(facets)
    slots = got.shape[1] - 2 * rows
    wide = 2 * S
    height = facets * rows
    column = lax.axis_index("col")
    sources = []
    for f in range(facets):
        re = got[f * cols, 0:rows, :].astype(F32)
        im = got[f * cols, rows : 2 * rows, :].astype(F32)
        for h in range(1, cols):
            re = re + got[f * cols + h, 0:rows, :].astype(F32)
            im = im + got[f * cols + h, rows : 2 * rows, :].astype(F32)
        left[f * rows : (f + 1) * rows, 0:W] = re
        left[f * rows : (f + 1) * rows, W : 2 * W] = im
        left[height + f * rows : height + (f + 1) * rows, 0:W] = im
        left[height + f * rows : height + (f + 1) * rows, W : 2 * W] = -re
        sources.append(got[f * cols + column, 2 * rows :, :].astype(F32))
    summed[...] = jnp.dot(left[...].astype(BF16), right[...], preferred_element_type=F32)
    heads = jnp.concatenate([note[0:1] for note in sources], axis=0)
    offset = (heads[:, W - 2 : W - 1] * 256.0 + heads[:, W - 1 : W]).astype(I32)
    lane = lax.broadcasted_iota(I32, (facets, wide), 1)
    cosine, sine = cos_sin(mod_phase(offset, positions(columns[0], lane)))
    phases[0] = cosine
    phases[1] = sine
    acc = jnp.zeros((rows, wide), F32)
    for f in range(facets):
        acc = acc + summed[f * rows : (f + 1) * rows, :] * phases[0, f : f + 1, :]
        acc = acc + summed[height + f * rows : height + (f + 1) * rows, :] * phases[1, f : f + 1, :]
    acc = acc * (1.0 / math.sqrt(facets))
    pieces = []
    for b in range(S // TILE):
        at = slice(b * 2 * TILE, (b + 1) * 2 * TILE)
        parts = [acc[i * tall : (i + 1) * tall, at] for i in range(inside)]
        if inside == 1:
            parts.append(jnp.zeros_like(parts[0]))
        pieces.append(jnp.concatenate(parts, axis=1))
    tiles = jnp.concatenate(pieces, axis=0).astype(BF16)
    names = jnp.concatenate(sources, axis=0).astype(I32)
    first = (lax.axis_index("facet") // (facets // groups)) * tall
    local = (names >> 3) - first
    wanted = jnp.where((local >= 0) & (local < tall), (names & 7) * tall + local, -1)
    count = tiles.shape[0]
    spot = lax.broadcasted_iota(I32, (facets * slots, W), 1)
    onehot = jnp.where(wanted == spot, 1.0, 0.0).astype(BF16)[:, 0:count]
    chosen = jnp.dot(onehot, tiles, preferred_element_type=F32)
    for o in range(facets):
        out[o] = chosen[o * slots : (o + 1) * slots, :].astype(BF16)


def across(got, right, columns, facets, cols):
    rows = S // facets
    slots = got.shape[1] - 2 * rows
    return pl.pallas_call(
        functools.partial(across_kernel, facets, cols),
        out_shape=jax.ShapeDtypeStruct((facets, slots, W), BF16),
        in_specs=[
            pl.BlockSpec(memory_space=pltpu.SMEM),
            pl.BlockSpec(memory_space=pltpu.VMEM),
            pl.BlockSpec(memory_space=pltpu.VMEM),
        ],
        out_specs=pl.BlockSpec(memory_space=pltpu.VMEM),
        scratch_shapes=[
            pltpu.VMEM((2 * S, 2 * W), F32),
            pltpu.VMEM((2 * S, 2 * S), F32),
            pltpu.VMEM((2, facets, 2 * S), F32),
        ],
        compiler_params=pltpu.CompilerParams(vmem_limit_bytes=VMEM_LIMIT),
        cost_estimate=pl.CostEstimate(
            flops=2 * 2 * S * 2 * W * 2 * S, bytes_accessed=1 << 20, transcendentals=0
        ),
        name="across",
    )(columns, got, right)


def waves_kernel(facets, live, uv, right, near, far):
    _, _, inside = split(facets)
    vis = uv.shape[2]
    step = NTOT // UV_STEPS
    line = lax.broadcasted_iota(I32, (TILE, vis), 0)
    low = line[0:8] * inside
    high = (line[0:4] % (4 // inside)) * 8 * inside + line[0:4] // (4 // inside)

    def slot(j, carry):
        cosine, sine = cos_sin((uv[j, 1:2, :] * (line * step)) & (NTOT - 1))
        cos_high, sin_high = cosine.astype(BF16), sine.astype(BF16)
        right[j, 0:TILE, :] = cos_high
        right[j, TILE : 2 * TILE, :] = sin_high
        right[j, 2 * TILE : 3 * TILE, :] = (cosine - cos_high.astype(F32)).astype(BF16)
        right[j, 3 * TILE : 4 * TILE, :] = (sine - sin_high.astype(F32)).astype(BF16)
        cosine, sine = cos_sin((uv[j, 0:1, :] * (low * step)) & (NTOT - 1))
        size = jnp.where(j < live[0, 0], 1.0 / TILE, 0.0)
        near[j, 0] = cosine * size
        near[j, 1] = sine * size
        cosine, sine = cos_sin((uv[j, 0:1, :] * (high * step)) & (NTOT - 1))
        far[j, 0] = cosine
        far[j, 1] = sine
        return carry

    lax.fori_loop(0, uv.shape[0], slot, 0)


def waves(live, uv, facets):
    slots, _, vis = uv.shape
    return pl.pallas_call(
        functools.partial(waves_kernel, facets),
        out_shape=(
            jax.ShapeDtypeStruct((slots, 4 * TILE, vis), BF16),
            jax.ShapeDtypeStruct((slots, 2, 8, vis), F32),
            jax.ShapeDtypeStruct((slots, 2, 4, vis), F32),
        ),
        in_specs=[
            pl.BlockSpec(memory_space=pltpu.SMEM),
            pl.BlockSpec(memory_space=pltpu.VMEM),
        ],
        out_specs=[pl.BlockSpec(memory_space=pltpu.VMEM)] * 3,
        compiler_params=pltpu.CompilerParams(vmem_limit_bytes=VMEM_LIMIT),
        cost_estimate=pl.CostEstimate(flops=1 << 26, bytes_accessed=3 << 20, transcendentals=0),
        name="waves",
    )(live, uv)


def visibility_kernel(facets, parts, right, near, far, out, held):
    groups, _, inside = split(facets)
    slots = out.shape[0]
    sources = facets // groups
    for f in range(sources):
        held[f] = parts[f].astype(F32)
        for g in range(1, groups):
            held[f] += parts[g * sources + f].astype(F32)
    lane = lax.broadcasted_iota(I32, (sources, W), 1)
    sign = jnp.where((lane & TILE) == 0, 1.0, -1.0).astype(F32)
    for j in range(slots):
        x = held[:, j, :]
        y = pltpu.roll(x, W // 2, 1)
        both = [jnp.where(lane < W // 2, x, y), jnp.where(lane < W // 2, y, x)][:inside]
        lhs = [z * sign for z in both] + [pltpu.roll(z, TILE, 1) for z in both]
        middle = jnp.dot(
            jnp.concatenate(lhs, axis=0).astype(BF16), right[j], preferred_element_type=F32
        )
        real, imag = middle[0:8], middle[TILE : TILE + 8]
        for h in range(1, 4):
            more_re = middle[8 * h : 8 * h + 8]
            more_im = middle[TILE + 8 * h : TILE + 8 * h + 8]
            cosine, sine = far[j, 0, h : h + 1, :], far[j, 1, h : h + 1, :]
            real = real + (cosine * more_re - sine * more_im)
            imag = imag + (cosine * more_im + sine * more_re)
        cosine, sine = near[j, 0], near[j, 1]
        out[j, 0:1, :] = jnp.sum(cosine * real - sine * imag, axis=0, keepdims=True)
        out[j, 1:2, :] = jnp.sum(cosine * imag + sine * real, axis=0, keepdims=True)


def visibilities_of(parts, tables, facets):
    slots, _, vis = tables[0].shape
    return pl.pallas_call(
        functools.partial(visibility_kernel, facets),
        out_shape=jax.ShapeDtypeStruct((slots, 2, vis), F32),
        in_specs=[pl.BlockSpec(memory_space=pltpu.VMEM)] * 4,
        out_specs=pl.BlockSpec(memory_space=pltpu.VMEM),
        scratch_shapes=[pltpu.VMEM((facets // split(facets)[0], slots, W), F32)],
        compiler_params=pltpu.CompilerParams(vmem_limit_bytes=VMEM_LIMIT),
        cost_estimate=pl.CostEstimate(
            flops=slots * 2 * 64 * 128 * vis, bytes_accessed=1 << 20, transcendentals=0
        ),
        name="visibility",
    )(parts, *tables)


def shards(
    facet_strips, facet_offsets, column_offsets, row_offsets, tile_lists, tile_counts, uv_index
):
    facets, cols = lax.axis_size("facet"), lax.axis_size("col")
    sent = along(facet_strips[0], row_offsets, facet_offsets, tile_lists, facets, cols)
    got = lax.all_to_all(sent, ("facet", "col"), 0, 0, tiled=True)
    right = base(column_offsets)
    tables = waves(tile_counts, uv_index[0, 0], facets)
    asked = across(got, right, column_offsets, facets, cols)
    parts = lax.all_to_all(asked, "facet", 0, 0, tiled=True)
    result = visibilities_of(parts, tables, facets)
    return result[None, None]


def solution(mesh):
    in_specs = (
        P("facet", None, "col", None),
        P("facet", None),
        P("col"),
        P(),
        P("col", "facet", None),
        P("col", "facet"),
        P("col", "facet", None, None, None),
    )
    out_specs = P("col", "facet", None, None, None)
    return jax.shard_map(shards, mesh=mesh, in_specs=in_specs, out_specs=out_specs, check_vma=False)
```

```python
import functools
import math

import jax
import jax.numpy as jnp
from jax import lax
from jax.experimental import pallas as pl
from jax.experimental.pallas import tpu as pltpu
from jax.sharding import PartitionSpec as P


L = 8192
W = 128
S = 256
TILE = 32
NTOT = 65536
UV_STEPS = 4096
VMEM_LIMIT = 16 << 20
CHUNK = 512
CHAIN = 16
AHEAD = 4
BF16 = jnp.bfloat16
F32 = jnp.float32
I32 = jnp.int32


def cos_sin(index):
    shifted = index + NTOT // 8
    quadrant = shifted >> 14
    rest = (shifted & (NTOT // 4 - 1)) - NTOT // 8
    x = rest.astype(F32) * (2.0 * math.pi / NTOT)
    y = x * x
    sine = x + x * (y * (-1.0 / 6 + y * (1.0 / 120 + y * (-1.0 / 5040 + y * (1.0 / 362880)))))
    cosine = 1.0 + y * (-0.5 + y * (1.0 / 24 + y * (-1.0 / 720 + y * (1.0 / 40320))))
    odd = (quadrant & 1) != 0
    first = jnp.where(odd, sine, cosine)
    second = jnp.where(odd, cosine, sine)
    return (
        jnp.where(((quadrant + 1) & 2) != 0, -first, first),
        jnp.where((quadrant & 2) != 0, -second, second),
    )


def mod_phase(first, second):
    return (first * second) & (NTOT - 1)


def split(facets):
    groups = max(1, facets // TILE)
    inside = TILE * groups // facets
    return groups, S // TILE // groups, inside


def along_kernel(facets, cols, chunk, scal, offsets, names, strip, out, held, table, total, state, outside, small, sems):
    count = held.shape[1]
    steps = count // chunk
    slots = names.shape[2]
    copies = []
    notes = []
    for n, (src, dst) in enumerate(zip((offsets, names), small)):
        notes.append(pltpu.make_async_copy(src, dst, sems.at[steps + n]))
        notes[n].start()
    for n in range(steps):
        part = pl.ds(n * chunk, chunk)
        copies.append(pltpu.make_async_copy(strip.at[:, part], held.at[:, part], sems.at[n]))
        copies[n].start()
    row_start = scal[0]
    rows = S // facets
    groups, tall, inside = split(facets)

    def sample_of(place):
        owner = place // rows
        within = place % rows
        group = owner // (facets // groups)
        line = (owner % (facets // groups)) * inside + within // tall
        return (within % tall + tall * group) * TILE + line

    blocks = S // 8
    inner = row_start + (NTOT // L) * sample_of(lax.broadcasted_iota(I32, (8, W), 0))
    outer = (NTOT // L) * sample_of(8 * lax.broadcasted_iota(I32, (blocks, W), 0))
    factors = {}

    def factor_tables(n, column, wide_column, scale):
        cosine, sine = cos_sin(mod_phase(inner, column))
        factors[n] = (cosine * scale, sine * scale)
        cosine, sine = cos_sin(mod_phase(outer, wide_column))
        outside[2 * n] = cosine
        outside[2 * n + 1] = sine

    def factor(n, k):
        cosine, sine = outside[2 * n, k : k + 1, :], outside[2 * n + 1, k : k + 1, :]
        x, y = factors[n]
        return x * cosine - y * sine, y * cosine + x * sine

    factor_tables(1, W, W, 1.0)
    factor_tables(2, CHAIN * W, CHAIN * W, 1.0)
    notes[0].wait()
    col_start = small[0][0, 0] + lax.axis_index("col") * count
    factor_tables(
        0,
        col_start + lax.broadcasted_iota(I32, (8, W), 1),
        col_start + lax.broadcasted_iota(I32, (blocks, W), 1),
        1.0 / math.sqrt(L),
    )

    def fill(n):
        slot = n % (AHEAD + 1)
        for k in range(blocks):
            at = slice(8 * k, 8 * k + 8)
            twice = None
            for local in range(chunk // W):
                stage = (n * (chunk // W) + local) % CHAIN
                if stage == 0:
                    if n == 0:
                        c1, s1 = factor(0, k)
                    else:
                        leap_c, leap_s = factor(2, k)
                        c0, s0 = state[4, at], state[5, at]
                        c1, s1 = c0 * leap_c - s0 * leap_s, s0 * leap_c + c0 * leap_s
                    if (n + 1) * chunk < count:
                        state[4, at], state[5, at] = c1, s1
                elif stage == 1:
                    turn_c, turn_s = factor(1, k)
                    twice = turn_c + turn_c
                    state[6, at] = twice
                    c0, s0 = c1, s1
                    c1, s1 = c0 * turn_c - s0 * turn_s, s0 * turn_c + c0 * turn_s
                else:
                    if twice is None:
                        twice = state[6, at]
                        c0, s0, c1, s1 = (state[i, at] for i in range(4))
                    c0, c1 = c1, twice * c1 - c0
                    s0, s1 = s1, twice * s1 - s0
                place = slice(local * W, (local + 1) * W)
                table[slot, at, place] = c1.astype(BF16)
                table[slot, S + 8 * k : S + 8 * k + 8, place] = s1.astype(BF16)
            if (n + 1) * (chunk // W) % CHAIN:
                for i, value in enumerate((c0, s0, c1, s1)):
                    state[i, at] = value

    ahead = min(AHEAD, steps)
    for n in range(ahead):
        fill(n)
    for copy in copies:
        copy.wait()
    for n in range(steps):
        if n + ahead < steps:
            fill(n + ahead)
        part = slice(n * chunk, (n + 1) * chunk)
        cells = jnp.concatenate([held[0, part, :], held[1, part, :]], axis=1)
        term = jnp.dot(table[n % (AHEAD + 1)], cells, preferred_element_type=F32)
        if n == 0:
            total[...] = term
        else:
            total[...] += term
    real = total[0:S, 0:W] + total[S : 2 * S, W : 2 * W]
    imag = total[0:S, W : 2 * W] - total[S : 2 * S, 0:W]
    total[0:S, 0:W] = real
    total[0:S, W : 2 * W] = imag
    notes[1].wait()
    across = small[0][0, 1]
    line = lax.broadcasted_iota(I32, (slots, W), 0)
    spot = lax.broadcasted_iota(I32, (slots, W), 1)
    note = jnp.zeros((slots, W), I32)
    for j in range(slots):
        note = jnp.where(line == j, small[1][0, 0, j], note)
    note = jnp.where(spot == W - 2, across >> 8, jnp.where(spot == W - 1, across & 255, note))
    note = note.astype(F32).astype(BF16)
    for o in range(facets):
        re = total[o * rows : (o + 1) * rows, 0:W].astype(BF16)
        im = total[o * rows : (o + 1) * rows, W : 2 * W].astype(BF16)
        for c in range(cols):
            out[o * cols + c, 0:rows, :] = re
            out[o * cols + c, rows : 2 * rows, :] = im
            out[o * cols + c, 2 * rows :, :] = note


def along(strip, row_offsets, facet_offsets, names, facets, cols):
    count = strip.shape[1]
    chunk = min(CHUNK, count)
    rows = S // facets
    slots = names.shape[2]
    return pl.pallas_call(
        functools.partial(along_kernel, facets, cols, chunk),
        out_shape=jax.ShapeDtypeStruct((facets * cols, 2 * rows + slots, W), BF16),
        in_specs=[pl.BlockSpec(memory_space=pltpu.SMEM)]
        + [pl.BlockSpec(memory_space=pltpu.HBM)] * 3,
        out_specs=pl.BlockSpec(memory_space=pltpu.VMEM),
        scratch_shapes=[
            pltpu.VMEM((2, count, W), BF16),
            pltpu.VMEM((AHEAD + 1, 2 * S, chunk), BF16),
            pltpu.VMEM((2 * S, 2 * W), F32),
            pltpu.VMEM((7, S, W), F32),
            pltpu.VMEM((6, S // 8, W), F32),
            [
                pltpu.SMEM(facet_offsets.shape, I32),
                pltpu.SMEM(names.shape, I32),
            ],
            pltpu.SemaphoreType.DMA((count // chunk + 2,)),
        ],
        cost_estimate=pl.CostEstimate(
            flops=8 * S * W * count, bytes_accessed=4 * count * W, transcendentals=0
        ),
        name="along",
    )(row_offsets, facet_offsets, names, strip)


def base_kernel(columns, out):
    cell = lax.broadcasted_iota(I32, (W, 2 * S), 0)
    lane = lax.broadcasted_iota(I32, (W, 2 * S), 1)
    turn = ((lane >> 5) & 1) * (NTOT // 4)
    top, bottom = cos_sin((cell * positions(columns[0], lane) + turn) & (NTOT - 1))
    scale = 1.0 / math.sqrt(W)
    out[0:W, :] = (top * scale).astype(BF16)
    out[W : 2 * W, :] = (bottom * scale).astype(BF16)


def positions(column, lane):
    return column + (NTOT // S) * ((lane >> 6) * TILE + (lane & (TILE - 1)))


def base(columns):
    return pl.pallas_call(
        base_kernel,
        out_shape=jax.ShapeDtypeStruct((2 * W, 2 * S), BF16),
        in_specs=[pl.BlockSpec(memory_space=pltpu.SMEM)],
        out_specs=pl.BlockSpec(memory_space=pltpu.VMEM),
        compiler_params=pltpu.CompilerParams(vmem_limit_bytes=VMEM_LIMIT),
        cost_estimate=pl.CostEstimate(flops=1 << 24, bytes_accessed=1 << 18, transcendentals=0),
        name="base",
    )(columns)


def across_kernel(facets, cols, columns, got, right, out, left, summed, phases):
    rows = S // facets
    groups, tall, inside = split(facets)
    slots = got.shape[1] - 2 * rows
    wide = 2 * S
    height = facets * rows
    column = lax.axis_index("col")
    sources = []
    for f in range(facets):
        re = got[f * cols, 0:rows, :].astype(F32)
        im = got[f * cols, rows : 2 * rows, :].astype(F32)
        for h in range(1, cols):
            re = re + got[f * cols + h, 0:rows, :].astype(F32)
            im = im + got[f * cols + h, rows : 2 * rows, :].astype(F32)
        left[f * rows : (f + 1) * rows, 0:W] = re
        left[f * rows : (f + 1) * rows, W : 2 * W] = im
        left[height + f * rows : height + (f + 1) * rows, 0:W] = im
        left[height + f * rows : height + (f + 1) * rows, W : 2 * W] = -re
        sources.append(got[f * cols + column, 2 * rows :, :].astype(F32))
    summed[...] = jnp.dot(left[...].astype(BF16), right[...], preferred_element_type=F32)
    heads = jnp.concatenate([note[0:1] for note in sources], axis=0)
    offset = (heads[:, W - 2 : W - 1] * 256.0 + heads[:, W - 1 : W]).astype(I32)
    lane = lax.broadcasted_iota(I32, (facets, wide), 1)
    cosine, sine = cos_sin(mod_phase(offset, positions(columns[0], lane)))
    phases[0] = cosine
    phases[1] = sine
    acc = jnp.zeros((rows, wide), F32)
    for f in range(facets):
        acc = acc + summed[f * rows : (f + 1) * rows, :] * phases[0, f : f + 1, :]
        acc = acc + summed[height + f * rows : height + (f + 1) * rows, :] * phases[1, f : f + 1, :]
    acc = acc * (1.0 / math.sqrt(facets))
    pieces = []
    for b in range(S // TILE):
        at = slice(b * 2 * TILE, (b + 1) * 2 * TILE)
        parts = [acc[i * tall : (i + 1) * tall, at] for i in range(inside)]
        if inside == 1:
            parts.append(jnp.zeros_like(parts[0]))
        pieces.append(jnp.concatenate(parts, axis=1))
    tiles = jnp.concatenate(pieces, axis=0).astype(BF16)
    names = jnp.concatenate(sources, axis=0).astype(I32)
    first = (lax.axis_index("facet") // (facets // groups)) * tall
    local = (names >> 3) - first
    wanted = jnp.where((local >= 0) & (local < tall), (names & 7) * tall + local, -1)
    count = tiles.shape[0]
    spot = lax.broadcasted_iota(I32, (facets * slots, W), 1)
    onehot = jnp.where(wanted == spot, 1.0, 0.0).astype(BF16)[:, 0:count]
    chosen = jnp.dot(onehot, tiles, preferred_element_type=F32)
    for o in range(facets):
        out[o] = chosen[o * slots : (o + 1) * slots, :].astype(BF16)


def across(got, right, columns, facets, cols):
    rows = S // facets
    slots = got.shape[1] - 2 * rows
    return pl.pallas_call(
        functools.partial(across_kernel, facets, cols),
        out_shape=jax.ShapeDtypeStruct((facets, slots, W), BF16),
        in_specs=[
            pl.BlockSpec(memory_space=pltpu.SMEM),
            pl.BlockSpec(memory_space=pltpu.VMEM),
            pl.BlockSpec(memory_space=pltpu.VMEM),
        ],
        out_specs=pl.BlockSpec(memory_space=pltpu.VMEM),
        scratch_shapes=[
            pltpu.VMEM((2 * S, 2 * W), F32),
            pltpu.VMEM((2 * S, 2 * S), F32),
            pltpu.VMEM((2, facets, 2 * S), F32),
        ],
        compiler_params=pltpu.CompilerParams(vmem_limit_bytes=VMEM_LIMIT),
        cost_estimate=pl.CostEstimate(
            flops=2 * 2 * S * 2 * W * 2 * S, bytes_accessed=1 << 20, transcendentals=0
        ),
        name="across",
    )(columns, got, right)


def waves_kernel(facets, live, uv, right, near, far):
    _, _, inside = split(facets)
    vis = uv.shape[2]
    step = NTOT // UV_STEPS
    line = lax.broadcasted_iota(I32, (TILE, vis), 0)
    low = line[0:8] * inside
    high = (line[0:4] % (4 // inside)) * 8 * inside + line[0:4] // (4 // inside)

    def slot(j, carry):
        cosine, sine = cos_sin((uv[j, 1:2, :] * (line * step)) & (NTOT - 1))
        cos_high, sin_high = cosine.astype(BF16), sine.astype(BF16)
        right[j, 0:TILE, :] = cos_high
        right[j, TILE : 2 * TILE, :] = sin_high
        right[j, 2 * TILE : 3 * TILE, :] = (cosine - cos_high.astype(F32)).astype(BF16)
        right[j, 3 * TILE : 4 * TILE, :] = (sine - sin_high.astype(F32)).astype(BF16)
        cosine, sine = cos_sin((uv[j, 0:1, :] * (low * step)) & (NTOT - 1))
        size = jnp.where(j < live[0, 0], 1.0 / TILE, 0.0)
        near[j, 0] = cosine * size
        near[j, 1] = sine * size
        cosine, sine = cos_sin((uv[j, 0:1, :] * (high * step)) & (NTOT - 1))
        far[j, 0] = cosine
        far[j, 1] = sine
        return carry

    lax.fori_loop(0, uv.shape[0], slot, 0)


def waves(live, uv, facets):
    slots, _, vis = uv.shape
    return pl.pallas_call(
        functools.partial(waves_kernel, facets),
        out_shape=(
            jax.ShapeDtypeStruct((slots, 4 * TILE, vis), BF16),
            jax.ShapeDtypeStruct((slots, 2, 8, vis), F32),
            jax.ShapeDtypeStruct((slots, 2, 4, vis), F32),
        ),
        in_specs=[
            pl.BlockSpec(memory_space=pltpu.SMEM),
            pl.BlockSpec(memory_space=pltpu.VMEM),
        ],
        out_specs=[pl.BlockSpec(memory_space=pltpu.VMEM)] * 3,
        compiler_params=pltpu.CompilerParams(vmem_limit_bytes=VMEM_LIMIT),
        cost_estimate=pl.CostEstimate(flops=1 << 26, bytes_accessed=3 << 20, transcendentals=0),
        name="waves",
    )(live, uv)


def visibility_kernel(facets, parts, right, near, far, out, held):
    groups, _, inside = split(facets)
    slots = out.shape[0]
    sources = facets // groups
    for f in range(sources):
        held[f] = parts[f].astype(F32)
        for g in range(1, groups):
            held[f] += parts[g * sources + f].astype(F32)
    lane = lax.broadcasted_iota(I32, (sources, W), 1)
    sign = jnp.where((lane & TILE) == 0, 1.0, -1.0).astype(F32)
    for j in range(slots):
        x = held[:, j, :]
        y = pltpu.roll(x, W // 2, 1)
        both = [jnp.where(lane < W // 2, x, y), jnp.where(lane < W // 2, y, x)][:inside]
        lhs = [z * sign for z in both] + [pltpu.roll(z, TILE, 1) for z in both]
        middle = jnp.dot(
            jnp.concatenate(lhs, axis=0).astype(BF16), right[j], preferred_element_type=F32
        )
        real, imag = middle[0:8], middle[TILE : TILE + 8]
        for h in range(1, 4):
            more_re = middle[8 * h : 8 * h + 8]
            more_im = middle[TILE + 8 * h : TILE + 8 * h + 8]
            cosine, sine = far[j, 0, h : h + 1, :], far[j, 1, h : h + 1, :]
            real = real + (cosine * more_re - sine * more_im)
            imag = imag + (cosine * more_im + sine * more_re)
        cosine, sine = near[j, 0], near[j, 1]
        out[j, 0:1, :] = jnp.sum(cosine * real - sine * imag, axis=0, keepdims=True)
        out[j, 1:2, :] = jnp.sum(cosine * imag + sine * real, axis=0, keepdims=True)


def visibilities_of(parts, tables, facets):
    slots, _, vis = tables[0].shape
    return pl.pallas_call(
        functools.partial(visibility_kernel, facets),
        out_shape=jax.ShapeDtypeStruct((slots, 2, vis), F32),
        in_specs=[pl.BlockSpec(memory_space=pltpu.VMEM)] * 4,
        out_specs=pl.BlockSpec(memory_space=pltpu.VMEM),
        scratch_shapes=[pltpu.VMEM((facets // split(facets)[0], slots, W), F32)],
        compiler_params=pltpu.CompilerParams(vmem_limit_bytes=VMEM_LIMIT),
        cost_estimate=pl.CostEstimate(
            flops=slots * 2 * 64 * 128 * vis, bytes_accessed=1 << 20, transcendentals=0
        ),
        name="visibility",
    )(parts, *tables)


def shards(
    facet_strips, facet_offsets, column_offsets, row_offsets, tile_lists, tile_counts, uv_index
):
    facets, cols = lax.axis_size("facet"), lax.axis_size("col")
    sent = along(facet_strips[0], row_offsets, facet_offsets, tile_lists, facets, cols)
    got = lax.all_to_all(sent, ("facet", "col"), 0, 0, tiled=True)
    right = base(column_offsets)
    tables = waves(tile_counts, uv_index[0, 0], facets)
    asked = across(got, right, column_offsets, facets, cols)
    parts = lax.all_to_all(asked, "facet", 0, 0, tiled=True)
    result = visibilities_of(parts, tables, facets)
    return result[None, None]


def solution(mesh):
    in_specs = (
        P("facet", None, "col", None),
        P("facet", None),
        P("col"),
        P(),
        P("col", "facet", None),
        P("col", "facet"),
        P("col", "facet", None, None, None),
    )
    out_specs = P("col", "facet", None, None, None)
    return jax.shard_map(shards, mesh=mesh, in_specs=in_specs, out_specs=out_specs, check_vma=False)
```

```python
import functools
import math

import jax
import jax.numpy as jnp
from jax import lax
from jax.experimental import pallas as pl
from jax.experimental.pallas import tpu as pltpu
from jax.sharding import PartitionSpec as P


L = 8192
W = 128
S = 256
TILE = 32
NTOT = 65536
UV_STEPS = 4096
VMEM_LIMIT = 16 << 20
CHUNK = 512
CHAIN = 16
AHEAD = 4
BF16 = jnp.bfloat16
F32 = jnp.float32
I32 = jnp.int32


def cos_sin(index):
    shifted = index + NTOT // 8
    quadrant = shifted >> 14
    rest = (shifted & (NTOT // 4 - 1)) - NTOT // 8
    x = rest.astype(F32) * (2.0 * math.pi / NTOT)
    y = x * x
    sine = x + x * (y * (-1.0 / 6 + y * (1.0 / 120 + y * (-1.0 / 5040 + y * (1.0 / 362880)))))
    cosine = 1.0 + y * (-0.5 + y * (1.0 / 24 + y * (-1.0 / 720 + y * (1.0 / 40320))))
    odd = (quadrant & 1) != 0
    first = jnp.where(odd, sine, cosine)
    second = jnp.where(odd, cosine, sine)
    return (
        jnp.where(((quadrant + 1) & 2) != 0, -first, first),
        jnp.where((quadrant & 2) != 0, -second, second),
    )


def mod_phase(first, second):
    return (first * second) & (NTOT - 1)


def split(facets):
    groups = max(1, facets // TILE)
    inside = TILE * groups // facets
    return groups, S // TILE // groups, inside


def along_kernel(facets, cols, chunk, scal, offsets, names, strip, out, held, table, total, state, outside, small, sems):
    count = held.shape[1]
    steps = count // chunk
    slots = names.shape[2]
    copies = []
    notes = []
    for n, (src, dst) in enumerate(zip((offsets, names), small)):
        notes.append(pltpu.make_async_copy(src, dst, sems.at[steps + n]))
        notes[n].start()
    for n in range(steps):
        part = pl.ds(n * chunk, chunk)
        copies.append(pltpu.make_async_copy(strip.at[:, part], held.at[:, part], sems.at[n]))
        copies[n].start()
    row_start = scal[0]
    rows = S // facets
    groups, tall, inside = split(facets)

    def sample_of(place):
        owner = place // rows
        within = place % rows
        group = owner // (facets // groups)
        line = (owner % (facets // groups)) * inside + within // tall
        return (within % tall + tall * group) * TILE + line

    blocks = S // 8
    inner = row_start + (NTOT // L) * sample_of(lax.broadcasted_iota(I32, (8, W), 0))
    outer = (NTOT // L) * sample_of(8 * lax.broadcasted_iota(I32, (blocks, W), 0))
    factors = {}

    def factor_tables(n, column, wide_column, scale):
        cosine, sine = cos_sin(mod_phase(inner, column))
        factors[n] = (cosine * scale, sine * scale)
        cosine, sine = cos_sin(mod_phase(outer, wide_column))
        outside[2 * n] = cosine
        outside[2 * n + 1] = sine

    def factor(n, k):
        cosine, sine = outside[2 * n, k : k + 1, :], outside[2 * n + 1, k : k + 1, :]
        x, y = factors[n]
        return x * cosine - y * sine, y * cosine + x * sine

    factor_tables(1, W, W, 1.0)
    factor_tables(2, CHAIN * W, CHAIN * W, 1.0)
    notes[0].wait()
    col_start = small[0][0, 0] + lax.axis_index("col") * count
    factor_tables(
        0,
        col_start + lax.broadcasted_iota(I32, (8, W), 1),
        col_start + lax.broadcasted_iota(I32, (blocks, W), 1),
        1.0 / math.sqrt(L),
    )

    def fill(n):
        slot = n % (AHEAD + 1)
        for k in range(blocks):
            at = slice(8 * k, 8 * k + 8)
            twice = None
            for local in range(chunk // W):
                stage = (n * (chunk // W) + local) % CHAIN
                if stage == 0:
                    if n == 0:
                        c1, s1 = factor(0, k)
                    else:
                        leap_c, leap_s = factor(2, k)
                        c0, s0 = state[4, at], state[5, at]
                        c1, s1 = c0 * leap_c - s0 * leap_s, s0 * leap_c + c0 * leap_s
                    if (n + 1) * chunk < count:
                        state[4, at], state[5, at] = c1, s1
                elif stage == 1:
                    turn_c, turn_s = factor(1, k)
                    twice = turn_c + turn_c
                    state[6, at] = twice
                    c0, s0 = c1, s1
                    c1, s1 = c0 * turn_c - s0 * turn_s, s0 * turn_c + c0 * turn_s
                else:
                    if twice is None:
                        twice = state[6, at]
                        c0, s0, c1, s1 = (state[i, at] for i in range(4))
                    c0, c1 = c1, twice * c1 - c0
                    s0, s1 = s1, twice * s1 - s0
                place = slice(local * W, (local + 1) * W)
                table[slot, at, place] = c1.astype(BF16)
                table[slot, S + 8 * k : S + 8 * k + 8, place] = s1.astype(BF16)
            if (n + 1) * (chunk // W) % CHAIN:
                for i, value in enumerate((c0, s0, c1, s1)):
                    state[i, at] = value

    ahead = min(AHEAD, steps)
    for n in range(ahead):
        fill(n)
    for copy in copies:
        copy.wait()
    for n in range(steps):
        if n + ahead < steps:
            fill(n + ahead)
        part = slice(n * chunk, (n + 1) * chunk)
        cells = jnp.concatenate([held[0, part, :], held[1, part, :]], axis=1)
        term = jnp.dot(table[n % (AHEAD + 1)], cells, preferred_element_type=F32)
        if n == 0:
            total[...] = term
        else:
            total[...] += term
    real = total[0:S, 0:W] + total[S : 2 * S, W : 2 * W]
    imag = total[0:S, W : 2 * W] - total[S : 2 * S, 0:W]
    total[0:S, 0:W] = real
    total[0:S, W : 2 * W] = imag
    notes[1].wait()
    across = small[0][0, 1]
    spot = lax.broadcasted_iota(I32, (2, W), 1)
    note = jnp.where(spot == W - 2, across >> 8, jnp.where(spot == W - 1, across & 255, 0))
    for j in range(slots):
        note = jnp.where(spot == j, small[1][0, 0, j], note)
    note = note.astype(F32).astype(BF16)
    for o in range(facets):
        re = total[o * rows : (o + 1) * rows, 0:W].astype(BF16)
        im = total[o * rows : (o + 1) * rows, W : 2 * W].astype(BF16)
        for c in range(cols):
            at = (o * cols + c) * (2 * rows + 2)
            out[at : at + rows, :] = re
            out[at + rows : at + 2 * rows, :] = im
            out[at + 2 * rows : at + 2 * rows + 2, :] = note


def along(strip, row_offsets, facet_offsets, names, facets, cols):
    count = strip.shape[1]
    chunk = min(CHUNK, count)
    rows = S // facets
    return pl.pallas_call(
        functools.partial(along_kernel, facets, cols, chunk),
        out_shape=jax.ShapeDtypeStruct((facets * cols * (2 * rows + 2), W), BF16),
        in_specs=[pl.BlockSpec(memory_space=pltpu.SMEM)]
        + [pl.BlockSpec(memory_space=pltpu.HBM)] * 3,
        out_specs=pl.BlockSpec(memory_space=pltpu.VMEM),
        scratch_shapes=[
            pltpu.VMEM((2, count, W), BF16),
            pltpu.VMEM((AHEAD + 1, 2 * S, chunk), BF16),
            pltpu.VMEM((2 * S, 2 * W), F32),
            pltpu.VMEM((7, S, W), F32),
            pltpu.VMEM((6, S // 8, W), F32),
            [
                pltpu.SMEM(facet_offsets.shape, I32),
                pltpu.SMEM(names.shape, I32),
            ],
            pltpu.SemaphoreType.DMA((count // chunk + 2,)),
        ],
        cost_estimate=pl.CostEstimate(
            flops=8 * S * W * count, bytes_accessed=4 * count * W, transcendentals=0
        ),
        name="along",
    )(row_offsets, facet_offsets, names, strip)


def base_kernel(columns, out):
    cell = lax.broadcasted_iota(I32, (W, 2 * S), 0)
    lane = lax.broadcasted_iota(I32, (W, 2 * S), 1)
    turn = ((lane >> 5) & 1) * (NTOT // 4)
    top, bottom = cos_sin((cell * positions(columns[0], lane) + turn) & (NTOT - 1))
    scale = 1.0 / math.sqrt(W)
    out[0:W, :] = (top * scale).astype(BF16)
    out[W : 2 * W, :] = (bottom * scale).astype(BF16)


def positions(column, lane):
    return column + (NTOT // S) * ((lane >> 6) * TILE + (lane & (TILE - 1)))


def base(columns):
    return pl.pallas_call(
        base_kernel,
        out_shape=jax.ShapeDtypeStruct((2 * W, 2 * S), BF16),
        in_specs=[pl.BlockSpec(memory_space=pltpu.SMEM)],
        out_specs=pl.BlockSpec(memory_space=pltpu.VMEM),
        compiler_params=pltpu.CompilerParams(vmem_limit_bytes=VMEM_LIMIT),
        cost_estimate=pl.CostEstimate(flops=1 << 24, bytes_accessed=1 << 18, transcendentals=0),
        name="base",
    )(columns)


def across_kernel(facets, cols, columns, got, right, out, left, summed, phases):
    rows = S // facets
    groups, tall, inside = split(facets)
    slots = out.shape[1]
    wide = 2 * S
    height = facets * rows
    size = 2 * rows + 2
    column = lax.axis_index("col")
    sources = []
    for f in range(facets):
        parts = []
        for part in range(2):
            at = f * cols * size + part * rows
            value = got[at : at + rows, :].astype(F32)
            for h in range(1, cols):
                value = value + got[at + h * size : at + h * size + rows, :].astype(F32)
            parts.append(value)
        re, im = parts
        left[f * rows : (f + 1) * rows, 0:W] = re
        left[f * rows : (f + 1) * rows, W : 2 * W] = im
        left[height + f * rows : height + (f + 1) * rows, 0:W] = im
        left[height + f * rows : height + (f + 1) * rows, W : 2 * W] = -re
        note = None
        for h in range(cols):
            at = (f * cols + h) * size + 2 * rows
            value = jnp.where(column == h, got[at : at + 2, :].astype(F32)[0:1], 0.0)
            note = value if note is None else note + value
        sources.append(note)
    summed[...] = jnp.dot(left[...].astype(BF16), right[...], preferred_element_type=F32)
    heads = jnp.concatenate(sources, axis=0)
    offset = (heads[:, W - 2 : W - 1] * 256.0 + heads[:, W - 1 : W]).astype(I32)
    lane = lax.broadcasted_iota(I32, (facets, wide), 1)
    cosine, sine = cos_sin(mod_phase(offset, positions(columns[0], lane)))
    phases[0] = cosine
    phases[1] = sine
    acc = jnp.zeros((rows, wide), F32)
    for f in range(facets):
        acc = acc + summed[f * rows : (f + 1) * rows, :] * phases[0, f : f + 1, :]
        acc = acc + summed[height + f * rows : height + (f + 1) * rows, :] * phases[1, f : f + 1, :]
    acc = acc * (1.0 / math.sqrt(facets))
    pieces = []
    for b in range(S // TILE):
        at = slice(b * 2 * TILE, (b + 1) * 2 * TILE)
        parts = [acc[i * tall : (i + 1) * tall, at] for i in range(inside)]
        if inside == 1:
            parts.append(jnp.zeros_like(parts[0]))
        pieces.append(jnp.concatenate(parts, axis=1))
    tiles = jnp.concatenate(pieces, axis=0).astype(BF16)
    line = lax.broadcasted_iota(I32, (facets * slots, facets), 0)
    place = line - slots * lax.broadcasted_iota(I32, line.shape, 1)
    owner = jnp.where((place >= 0) & (place < slots), 1.0, 0.0)
    spread = jnp.dot(owner.astype(BF16), heads.astype(BF16), preferred_element_type=F32)
    line = lax.broadcasted_iota(I32, spread.shape, 0)
    own = lax.broadcasted_iota(I32, spread.shape, 1) == (line & (slots - 1))
    names = jnp.sum(jnp.where(own, spread, 0.0), axis=1, keepdims=True).astype(I32)
    first = (lax.axis_index("facet") // (facets // groups)) * tall
    local = (names >> 3) - first
    wanted = jnp.where((local >= 0) & (local < tall), (names & 7) * tall + local, -1)
    count = tiles.shape[0]
    spot = lax.broadcasted_iota(I32, (facets * slots, W), 1)
    onehot = jnp.where(wanted == spot, 1.0, 0.0).astype(BF16)[:, 0:count]
    chosen = jnp.dot(onehot, tiles, preferred_element_type=F32)
    for o in range(facets):
        out[o] = chosen[o * slots : (o + 1) * slots, :].astype(BF16)


def across(got, right, columns, slots, facets, cols):
    return pl.pallas_call(
        functools.partial(across_kernel, facets, cols),
        out_shape=jax.ShapeDtypeStruct((facets, slots, W), BF16),
        in_specs=[
            pl.BlockSpec(memory_space=pltpu.SMEM),
            pl.BlockSpec(memory_space=pltpu.VMEM),
            pl.BlockSpec(memory_space=pltpu.VMEM),
        ],
        out_specs=pl.BlockSpec(memory_space=pltpu.VMEM),
        scratch_shapes=[
            pltpu.VMEM((2 * S, 2 * W), F32),
            pltpu.VMEM((2 * S, 2 * S), F32),
            pltpu.VMEM((2, facets, 2 * S), F32),
        ],
        compiler_params=pltpu.CompilerParams(vmem_limit_bytes=VMEM_LIMIT),
        cost_estimate=pl.CostEstimate(
            flops=2 * 2 * S * 2 * W * 2 * S, bytes_accessed=1 << 20, transcendentals=0
        ),
        name="across",
    )(columns, got, right)


def waves_kernel(facets, live, uv, right, near, far):
    _, _, inside = split(facets)
    vis = uv.shape[2]
    step = NTOT // UV_STEPS
    line = lax.broadcasted_iota(I32, (TILE, vis), 0)
    low = line[0:8] * inside
    high = (line[0:4] % (4 // inside)) * 8 * inside + line[0:4] // (4 // inside)

    def slot(j, carry):
        cosine, sine = cos_sin((uv[j, 1:2, :] * (line * step)) & (NTOT - 1))
        cos_high, sin_high = cosine.astype(BF16), sine.astype(BF16)
        right[j, 0:TILE, :] = cos_high
        right[j, TILE : 2 * TILE, :] = sin_high
        right[j, 2 * TILE : 3 * TILE, :] = (cosine - cos_high.astype(F32)).astype(BF16)
        right[j, 3 * TILE : 4 * TILE, :] = (sine - sin_high.astype(F32)).astype(BF16)
        cosine, sine = cos_sin((uv[j, 0:1, :] * (low * step)) & (NTOT - 1))
        size = jnp.where(j < live[0, 0], 1.0 / TILE, 0.0)
        near[j, 0] = cosine * size
        near[j, 1] = sine * size
        cosine, sine = cos_sin((uv[j, 0:1, :] * (high * step)) & (NTOT - 1))
        far[j, 0] = cosine
        far[j, 1] = sine
        return carry

    lax.fori_loop(0, uv.shape[0], slot, 0)


def waves(live, uv, facets):
    slots, _, vis = uv.shape
    return pl.pallas_call(
        functools.partial(waves_kernel, facets),
        out_shape=(
            jax.ShapeDtypeStruct((slots, 4 * TILE, vis), BF16),
            jax.ShapeDtypeStruct((slots, 2, 8, vis), F32),
            jax.ShapeDtypeStruct((slots, 2, 4, vis), F32),
        ),
        in_specs=[
            pl.BlockSpec(memory_space=pltpu.SMEM),
            pl.BlockSpec(memory_space=pltpu.VMEM),
        ],
        out_specs=[pl.BlockSpec(memory_space=pltpu.VMEM)] * 3,
        compiler_params=pltpu.CompilerParams(vmem_limit_bytes=VMEM_LIMIT),
        cost_estimate=pl.CostEstimate(flops=1 << 26, bytes_accessed=3 << 20, transcendentals=0),
        name="waves",
    )(live, uv)


def visibility_kernel(facets, parts, right, near, far, out, held):
    groups, _, inside = split(facets)
    slots = out.shape[0]
    sources = facets // groups
    for f in range(sources):
        held[f] = parts[f].astype(F32)
        for g in range(1, groups):
            held[f] += parts[g * sources + f].astype(F32)
    lane = lax.broadcasted_iota(I32, (sources, W), 1)
    sign = jnp.where((lane & TILE) == 0, 1.0, -1.0).astype(F32)
    for j in range(slots):
        x = held[:, j, :]
        y = pltpu.roll(x, W // 2, 1)
        both = [jnp.where(lane < W // 2, x, y), jnp.where(lane < W // 2, y, x)][:inside]
        lhs = [z * sign for z in both] + [pltpu.roll(z, TILE, 1) for z in both]
        middle = jnp.dot(
            jnp.concatenate(lhs, axis=0).astype(BF16), right[j], preferred_element_type=F32
        )
        real, imag = middle[0:8], middle[TILE : TILE + 8]
        for h in range(1, 4):
            more_re = middle[8 * h : 8 * h + 8]
            more_im = middle[TILE + 8 * h : TILE + 8 * h + 8]
            cosine, sine = far[j, 0, h : h + 1, :], far[j, 1, h : h + 1, :]
            real = real + (cosine * more_re - sine * more_im)
            imag = imag + (cosine * more_im + sine * more_re)
        cosine, sine = near[j, 0], near[j, 1]
        out[j, 0:1, :] = jnp.sum(cosine * real - sine * imag, axis=0, keepdims=True)
        out[j, 1:2, :] = jnp.sum(cosine * imag + sine * real, axis=0, keepdims=True)


def visibilities_of(parts, tables, facets):
    slots, _, vis = tables[0].shape
    return pl.pallas_call(
        functools.partial(visibility_kernel, facets),
        out_shape=jax.ShapeDtypeStruct((slots, 2, vis), F32),
        in_specs=[pl.BlockSpec(memory_space=pltpu.VMEM)] * 4,
        out_specs=pl.BlockSpec(memory_space=pltpu.VMEM),
        scratch_shapes=[pltpu.VMEM((facets // split(facets)[0], slots, W), F32)],
        compiler_params=pltpu.CompilerParams(vmem_limit_bytes=VMEM_LIMIT),
        cost_estimate=pl.CostEstimate(
            flops=slots * 2 * 64 * 128 * vis, bytes_accessed=1 << 20, transcendentals=0
        ),
        name="visibility",
    )(parts, *tables)


def shards(
    facet_strips, facet_offsets, column_offsets, row_offsets, tile_lists, tile_counts, uv_index
):
    facets, cols = lax.axis_size("facet"), lax.axis_size("col")
    sent = along(facet_strips[0], row_offsets, facet_offsets, tile_lists, facets, cols)
    pairs = sent.reshape((facets * cols, -1, 2, W))
    got = lax.all_to_all(pairs, ("facet", "col"), 0, 0, tiled=True)
    got = got.reshape(sent.shape)
    right = base(column_offsets)
    tables = waves(tile_counts, uv_index[0, 0], facets)
    asked = across(got, right, column_offsets, tile_lists.shape[2], facets, cols)
    parts = lax.all_to_all(asked, "facet", 0, 0, tiled=True)
    result = visibilities_of(parts, tables, facets)
    return result[None, None]


def solution(mesh):
    in_specs = (
        P("facet", None, "col", None),
        P("facet", None),
        P("col"),
        P(),
        P("col", "facet", None),
        P("col", "facet"),
        P("col", "facet", None, None, None),
    )
    out_specs = P("col", "facet", None, None, None)
    return jax.shard_map(shards, mesh=mesh, in_specs=in_specs, out_specs=out_specs, check_vma=False)
```

```python
import functools
import math

import jax
import jax.numpy as jnp
from jax import lax
from jax.experimental import pallas as pl
from jax.experimental.pallas import tpu as pltpu
from jax.sharding import PartitionSpec as P


L = 8192
W = 128
S = 256
TILE = 32
NTOT = 65536
UV_STEPS = 4096
VMEM_LIMIT = 16 << 20
CHUNK = 4096
CHAIN = 32
AHEAD = 1
BF16 = jnp.bfloat16
F32 = jnp.float32
I32 = jnp.int32


def cos_sin(index):
    shifted = index + NTOT // 8
    quadrant = shifted >> 14
    rest = (shifted & (NTOT // 4 - 1)) - NTOT // 8
    x = rest.astype(F32) * (2.0 * math.pi / NTOT)
    y = x * x
    sine = x + x * (y * (-1.0 / 6 + y * (1.0 / 120 + y * (-1.0 / 5040 + y * (1.0 / 362880)))))
    cosine = 1.0 + y * (-0.5 + y * (1.0 / 24 + y * (-1.0 / 720 + y * (1.0 / 40320))))
    odd = (quadrant & 1) != 0
    first = jnp.where(odd, sine, cosine)
    second = jnp.where(odd, cosine, sine)
    return (
        jnp.where(((quadrant + 1) & 2) != 0, -first, first),
        jnp.where((quadrant & 2) != 0, -second, second),
    )


def mod_phase(first, second):
    return (first * second) & (NTOT - 1)


def split(facets):
    groups = max(1, facets // TILE)
    inside = TILE * groups // facets
    return groups, S // TILE // groups, inside


def along_kernel(facets, cols, chunk, scal, offsets, names, strip, out, held, table, total, state, outside, small, sems):
    count = held.shape[1]
    steps = count // chunk
    slots = names.shape[2]
    copies = []
    notes = []
    for n, (src, dst) in enumerate(zip((offsets, names), small)):
        notes.append(pltpu.make_async_copy(src, dst, sems.at[steps + n]))
        notes[n].start()
    for n in range(steps):
        part = pl.ds(n * chunk, chunk)
        copies.append(pltpu.make_async_copy(strip.at[:, part], held.at[:, part], sems.at[n]))
        copies[n].start()
    row_start = scal[0]
    rows = S // facets
    groups, tall, inside = split(facets)

    def sample_of(place):
        owner = place // rows
        within = place % rows
        group = owner // (facets // groups)
        line = (owner % (facets // groups)) * inside + within // tall
        return (within % tall + tall * group) * TILE + line

    blocks = S // 8
    inner = row_start + (NTOT // L) * sample_of(lax.broadcasted_iota(I32, (8, W), 0))
    outer = (NTOT // L) * sample_of(8 * lax.broadcasted_iota(I32, (blocks, W), 0))
    factors = {}

    def factor_tables(n, column, wide_column, scale):
        cosine, sine = cos_sin(mod_phase(inner, column))
        factors[n] = (cosine * scale, sine * scale)
        cosine, sine = cos_sin(mod_phase(outer, wide_column))
        outside[2 * n] = cosine
        outside[2 * n + 1] = sine

    def factor(n, k):
        cosine, sine = outside[2 * n, k : k + 1, :], outside[2 * n + 1, k : k + 1, :]
        x, y = factors[n]
        return x * cosine - y * sine, y * cosine + x * sine

    factor_tables(1, W, W, 1.0)
    factor_tables(2, CHAIN * W, CHAIN * W, 1.0)
    notes[0].wait()
    col_start = small[0][0, 0] + lax.axis_index("col") * count
    factor_tables(
        0,
        col_start + lax.broadcasted_iota(I32, (8, W), 1),
        col_start + lax.broadcasted_iota(I32, (blocks, W), 1),
        1.0 / math.sqrt(L),
    )

    def fill(n):
        slot = n % (AHEAD + 1)
        for k in range(blocks):
            at = slice(8 * k, 8 * k + 8)
            twice = None
            for local in range(chunk // W):
                stage = (n * (chunk // W) + local) % CHAIN
                if stage == 0:
                    if n == 0:
                        c1, s1 = factor(0, k)
                    else:
                        leap_c, leap_s = factor(2, k)
                        c0, s0 = state[4, at], state[5, at]
                        c1, s1 = c0 * leap_c - s0 * leap_s, s0 * leap_c + c0 * leap_s
                    if (n + 1) * chunk < count:
                        state[4, at], state[5, at] = c1, s1
                elif stage == 1:
                    turn_c, turn_s = factor(1, k)
                    twice = turn_c + turn_c
                    state[6, at] = twice
                    c0, s0 = c1, s1
                    c1, s1 = c0 * turn_c - s0 * turn_s, s0 * turn_c + c0 * turn_s
                else:
                    if twice is None:
                        twice = state[6, at]
                        c0, s0, c1, s1 = (state[i, at] for i in range(4))
                    c0, c1 = c1, twice * c1 - c0
                    s0, s1 = s1, twice * s1 - s0
                place = slice(local * W, (local + 1) * W)
                table[slot, at, place] = c1.astype(BF16)
                table[slot, S + 8 * k : S + 8 * k + 8, place] = s1.astype(BF16)
            if (n + 1) * (chunk // W) % CHAIN:
                for i, value in enumerate((c0, s0, c1, s1)):
                    state[i, at] = value

    ahead = min(AHEAD, steps)
    for n in range(ahead):
        fill(n)
    for copy in copies:
        copy.wait()
    for n in range(steps):
        if n + ahead < steps:
            fill(n + ahead)
        part = slice(n * chunk, (n + 1) * chunk)
        cells = jnp.concatenate([held[0, part, :], held[1, part, :]], axis=1)
        for at in (slice(0, S), slice(S, 2 * S)):
            term = jnp.dot(table[n % (AHEAD + 1), at, :], cells, preferred_element_type=F32)
            if n == 0:
                total[at, :] = term
            else:
                total[at, :] += term
    real = total[0:S, 0:W] + total[S : 2 * S, W : 2 * W]
    imag = total[0:S, W : 2 * W] - total[S : 2 * S, 0:W]
    total[0:S, 0:W] = real
    total[0:S, W : 2 * W] = imag
    notes[1].wait()
    across = small[0][0, 1]
    spot = lax.broadcasted_iota(I32, (2, W), 1)
    note = jnp.where(spot == W - 2, across >> 8, jnp.where(spot == W - 1, across & 255, 0))
    for j in range(slots):
        note = jnp.where(spot == j, small[1][0, 0, j], note)
    note = note.astype(F32).astype(BF16)
    for o in range(facets):
        re = total[o * rows : (o + 1) * rows, 0:W].astype(BF16)
        im = total[o * rows : (o + 1) * rows, W : 2 * W].astype(BF16)
        for c in range(cols):
            at = (c * facets + o) * (2 * rows + 2)
            out[at : at + rows, :] = re
            out[at + rows : at + 2 * rows, :] = im
            out[at + 2 * rows : at + 2 * rows + 2, :] = note


def along(strip, row_offsets, facet_offsets, names, facets, cols):
    count = strip.shape[1]
    chunk = min(CHUNK, count)
    rows = S // facets
    return pl.pallas_call(
        functools.partial(along_kernel, facets, cols, chunk),
        out_shape=jax.ShapeDtypeStruct((facets * cols * (2 * rows + 2), W), BF16),
        in_specs=[pl.BlockSpec(memory_space=pltpu.SMEM)]
        + [pl.BlockSpec(memory_space=pltpu.HBM)] * 3,
        out_specs=pl.BlockSpec(memory_space=pltpu.VMEM),
        scratch_shapes=[
            pltpu.VMEM((2, count, W), BF16),
            pltpu.VMEM((AHEAD + 1, 2 * S, chunk), BF16),
            pltpu.VMEM((2 * S, 2 * W), F32),
            pltpu.VMEM((7, S, W), F32),
            pltpu.VMEM((6, S // 8, W), F32),
            [
                pltpu.SMEM(facet_offsets.shape, I32),
                pltpu.SMEM(names.shape, I32),
            ],
            pltpu.SemaphoreType.DMA((count // chunk + 2,)),
        ],
        cost_estimate=pl.CostEstimate(
            flops=8 * S * W * count, bytes_accessed=4 * count * W, transcendentals=0
        ),
        name="along",
    )(row_offsets, facet_offsets, names, strip)


def base_kernel(columns, out):
    cell = lax.broadcasted_iota(I32, (W, 2 * S), 0)
    lane = lax.broadcasted_iota(I32, (W, 2 * S), 1)
    turn = ((lane >> 5) & 1) * (NTOT // 4)
    top, bottom = cos_sin((cell * positions(columns[0], lane) + turn) & (NTOT - 1))
    scale = 1.0 / math.sqrt(W)
    out[0:W, :] = (top * scale).astype(BF16)
    out[W : 2 * W, :] = (bottom * scale).astype(BF16)


def positions(column, lane):
    return column + (NTOT // S) * ((lane >> 6) * TILE + (lane & (TILE - 1)))


def base(columns):
    return pl.pallas_call(
        base_kernel,
        out_shape=jax.ShapeDtypeStruct((2 * W, 2 * S), BF16),
        in_specs=[pl.BlockSpec(memory_space=pltpu.SMEM)],
        out_specs=pl.BlockSpec(memory_space=pltpu.VMEM),
        compiler_params=pltpu.CompilerParams(vmem_limit_bytes=VMEM_LIMIT),
        cost_estimate=pl.CostEstimate(flops=1 << 24, bytes_accessed=1 << 18, transcendentals=0),
        name="base",
    )(columns)


def across_kernel(facets, cols, columns, got, right, out, left, summed, phases):
    rows = S // facets
    groups, tall, inside = split(facets)
    slots = out.shape[1]
    wide = 2 * S
    height = facets * rows
    size = 2 * rows + 2
    column = lax.axis_index("col")
    sources = []
    for f in range(facets):
        parts = []
        for part in range(2):
            at = f * size + part * rows
            value = got[at : at + rows, :].astype(F32)
            for h in range(1, cols):
                step = at + h * facets * size
                value = value + got[step : step + rows, :].astype(F32)
            parts.append(value)
        re, im = parts
        left[f * rows : (f + 1) * rows, 0:W] = re
        left[f * rows : (f + 1) * rows, W : 2 * W] = im
        left[height + f * rows : height + (f + 1) * rows, 0:W] = im
        left[height + f * rows : height + (f + 1) * rows, W : 2 * W] = -re
        note = None
        for h in range(cols):
            at = (h * facets + f) * size + 2 * rows
            value = jnp.where(column == h, got[at : at + 2, :].astype(F32)[0:1], 0.0)
            note = value if note is None else note + value
        sources.append(note)
    summed[...] = jnp.dot(left[...].astype(BF16), right[...], preferred_element_type=F32)
    heads = jnp.concatenate(sources, axis=0)
    offset = (heads[:, W - 2 : W - 1] * 256.0 + heads[:, W - 1 : W]).astype(I32)
    lane = lax.broadcasted_iota(I32, (facets, wide), 1)
    cosine, sine = cos_sin(mod_phase(offset, positions(columns[0], lane)))
    phases[0] = cosine
    phases[1] = sine
    acc = jnp.zeros((rows, wide), F32)
    for f in range(facets):
        acc = acc + summed[f * rows : (f + 1) * rows, :] * phases[0, f : f + 1, :]
        acc = acc + summed[height + f * rows : height + (f + 1) * rows, :] * phases[1, f : f + 1, :]
    acc = acc * (1.0 / math.sqrt(facets))
    pieces = []
    for b in range(S // TILE):
        at = slice(b * 2 * TILE, (b + 1) * 2 * TILE)
        parts = [acc[i * tall : (i + 1) * tall, at] for i in range(inside)]
        if inside == 1:
            parts.append(jnp.zeros_like(parts[0]))
        pieces.append(jnp.concatenate(parts, axis=1))
    tiles = jnp.concatenate(pieces, axis=0).astype(BF16)
    line = lax.broadcasted_iota(I32, (facets * slots, facets), 0)
    place = line - slots * lax.broadcasted_iota(I32, line.shape, 1)
    owner = jnp.where((place >= 0) & (place < slots), 1.0, 0.0)
    spread = jnp.dot(owner.astype(BF16), heads.astype(BF16), preferred_element_type=F32)
    line = lax.broadcasted_iota(I32, spread.shape, 0)
    own = lax.broadcasted_iota(I32, spread.shape, 1) == (line & (slots - 1))
    names = jnp.sum(jnp.where(own, spread, 0.0), axis=1, keepdims=True).astype(I32)
    first = (lax.axis_index("facet") // (facets // groups)) * tall
    local = (names >> 3) - first
    wanted = jnp.where((local >= 0) & (local < tall), (names & 7) * tall + local, -1)
    count = tiles.shape[0]
    spot = lax.broadcasted_iota(I32, (facets * slots, W), 1)
    onehot = jnp.where(wanted == spot, 1.0, 0.0).astype(BF16)[:, 0:count]
    chosen = jnp.dot(onehot, tiles, preferred_element_type=F32)
    for o in range(facets):
        out[o] = chosen[o * slots : (o + 1) * slots, :].astype(BF16)


def across(got, right, columns, slots, facets, cols):
    return pl.pallas_call(
        functools.partial(across_kernel, facets, cols),
        out_shape=jax.ShapeDtypeStruct((facets, slots, W), BF16),
        in_specs=[
            pl.BlockSpec(memory_space=pltpu.SMEM),
            pl.BlockSpec(memory_space=pltpu.VMEM),
            pl.BlockSpec(memory_space=pltpu.VMEM),
        ],
        out_specs=pl.BlockSpec(memory_space=pltpu.VMEM),
        scratch_shapes=[
            pltpu.VMEM((2 * S, 2 * W), F32),
            pltpu.VMEM((2 * S, 2 * S), F32),
            pltpu.VMEM((2, facets, 2 * S), F32),
        ],
        compiler_params=pltpu.CompilerParams(vmem_limit_bytes=VMEM_LIMIT),
        cost_estimate=pl.CostEstimate(
            flops=2 * 2 * S * 2 * W * 2 * S, bytes_accessed=1 << 20, transcendentals=0
        ),
        name="across",
    )(columns, got, right)


def waves_kernel(facets, live, uv, right, near, far):
    _, _, inside = split(facets)
    vis = uv.shape[2]
    step = NTOT // UV_STEPS
    line = lax.broadcasted_iota(I32, (TILE, vis), 0)
    low = line[0:8] * inside
    high = (line[0:4] % (4 // inside)) * 8 * inside + line[0:4] // (4 // inside)

    def slot(j, carry):
        cosine, sine = cos_sin((uv[j, 1:2, :] * (line * step)) & (NTOT - 1))
        cos_high, sin_high = cosine.astype(BF16), sine.astype(BF16)
        right[j, 0:TILE, :] = cos_high
        right[j, TILE : 2 * TILE, :] = sin_high
        right[j, 2 * TILE : 3 * TILE, :] = (cosine - cos_high.astype(F32)).astype(BF16)
        right[j, 3 * TILE : 4 * TILE, :] = (sine - sin_high.astype(F32)).astype(BF16)
        cosine, sine = cos_sin((uv[j, 0:1, :] * (low * step)) & (NTOT - 1))
        size = jnp.where(j < live[0, 0], 1.0 / TILE, 0.0)
        near[j, 0] = cosine * size
        near[j, 1] = sine * size
        cosine, sine = cos_sin((uv[j, 0:1, :] * (high * step)) & (NTOT - 1))
        far[j, 0] = cosine
        far[j, 1] = sine
        return carry

    lax.fori_loop(0, uv.shape[0], slot, 0)


def waves(live, uv, facets):
    slots, _, vis = uv.shape
    return pl.pallas_call(
        functools.partial(waves_kernel, facets),
        out_shape=(
            jax.ShapeDtypeStruct((slots, 4 * TILE, vis), BF16),
            jax.ShapeDtypeStruct((slots, 2, 8, vis), F32),
            jax.ShapeDtypeStruct((slots, 2, 4, vis), F32),
        ),
        in_specs=[
            pl.BlockSpec(memory_space=pltpu.SMEM),
            pl.BlockSpec(memory_space=pltpu.VMEM),
        ],
        out_specs=[pl.BlockSpec(memory_space=pltpu.VMEM)] * 3,
        compiler_params=pltpu.CompilerParams(vmem_limit_bytes=VMEM_LIMIT),
        cost_estimate=pl.CostEstimate(flops=1 << 26, bytes_accessed=3 << 20, transcendentals=0),
        name="waves",
    )(live, uv)


def visibility_kernel(facets, parts, right, near, far, out, held):
    groups, _, inside = split(facets)
    slots = out.shape[0]
    sources = facets // groups
    for f in range(sources):
        held[f] = parts[f].astype(F32)
        for g in range(1, groups):
            held[f] += parts[g * sources + f].astype(F32)
    lane = lax.broadcasted_iota(I32, (sources, W), 1)
    sign = jnp.where((lane & TILE) == 0, 1.0, -1.0).astype(F32)
    for j in range(slots):
        x = held[:, j, :]
        y = pltpu.roll(x, W // 2, 1)
        both = [jnp.where(lane < W // 2, x, y), jnp.where(lane < W // 2, y, x)][:inside]
        lhs = [z * sign for z in both] + [pltpu.roll(z, TILE, 1) for z in both]
        middle = jnp.dot(
            jnp.concatenate(lhs, axis=0).astype(BF16), right[j], preferred_element_type=F32
        )
        real, imag = middle[0:8], middle[TILE : TILE + 8]
        for h in range(1, 4):
            more_re = middle[8 * h : 8 * h + 8]
            more_im = middle[TILE + 8 * h : TILE + 8 * h + 8]
            cosine, sine = far[j, 0, h : h + 1, :], far[j, 1, h : h + 1, :]
            real = real + (cosine * more_re - sine * more_im)
            imag = imag + (cosine * more_im + sine * more_re)
        cosine, sine = near[j, 0], near[j, 1]
        out[j, 0:1, :] = jnp.sum(cosine * real - sine * imag, axis=0, keepdims=True)
        out[j, 1:2, :] = jnp.sum(cosine * imag + sine * real, axis=0, keepdims=True)


def visibilities_of(parts, tables, facets):
    slots, _, vis = tables[0].shape
    return pl.pallas_call(
        functools.partial(visibility_kernel, facets),
        out_shape=jax.ShapeDtypeStruct((slots, 2, vis), F32),
        in_specs=[pl.BlockSpec(memory_space=pltpu.VMEM)] * 4,
        out_specs=pl.BlockSpec(memory_space=pltpu.VMEM),
        scratch_shapes=[pltpu.VMEM((facets // split(facets)[0], slots, W), F32)],
        compiler_params=pltpu.CompilerParams(vmem_limit_bytes=VMEM_LIMIT),
        cost_estimate=pl.CostEstimate(
            flops=slots * 2 * 64 * 128 * vis, bytes_accessed=1 << 20, transcendentals=0
        ),
        name="visibility",
    )(parts, *tables)


def shards(
    facet_strips, facet_offsets, column_offsets, row_offsets, tile_lists, tile_counts, uv_index
):
    facets, cols = lax.axis_size("facet"), lax.axis_size("col")
    sent = along(facet_strips[0], row_offsets, facet_offsets, tile_lists, facets, cols)
    pairs = sent.reshape((facets * cols, -1, 2, W))
    got = lax.all_to_all(pairs, ("col", "facet"), 0, 0, tiled=True)
    got = got.reshape(sent.shape)
    right = base(column_offsets)
    tables = waves(tile_counts, uv_index[0, 0], facets)
    asked = across(got, right, column_offsets, tile_lists.shape[2], facets, cols)
    parts = lax.all_to_all(asked, "facet", 0, 0, tiled=True)
    result = visibilities_of(parts, tables, facets)
    return result[None, None]


def solution(mesh):
    in_specs = (
        P("facet", None, "col", None),
        P("facet", None),
        P("col"),
        P(),
        P("col", "facet", None),
        P("col", "facet"),
        P("col", "facet", None, None, None),
    )
    out_specs = P("col", "facet", None, None, None)
    return jax.shard_map(shards, mesh=mesh, in_specs=in_specs, out_specs=out_specs, check_vma=False)
```

```python
import functools
import math

import jax
import jax.numpy as jnp
from jax import lax
from jax.experimental import pallas as pl
from jax.experimental.pallas import tpu as pltpu
from jax.sharding import PartitionSpec as P


L = 8192
W = 128
S = 256
TILE = 32
NTOT = 65536
UV_STEPS = 4096
VMEM_LIMIT = 16 << 20
CHUNK = 2048
BF16 = jnp.bfloat16
F32 = jnp.float32
I32 = jnp.int32


def cos_sin(index):
    shifted = index + NTOT // 8
    quadrant = shifted >> 14
    rest = (shifted & (NTOT // 4 - 1)) - NTOT // 8
    x = rest.astype(F32) * (2.0 * math.pi / NTOT)
    y = x * x
    sine = x + x * (y * (-1.0 / 6 + y * (1.0 / 120 + y * (-1.0 / 5040 + y * (1.0 / 362880)))))
    cosine = 1.0 + y * (-0.5 + y * (1.0 / 24 + y * (-1.0 / 720 + y * (1.0 / 40320))))
    odd = (quadrant & 1) != 0
    first = jnp.where(odd, sine, cosine)
    second = jnp.where(odd, cosine, sine)
    return (
        jnp.where(((quadrant + 1) & 2) != 0, -first, first),
        jnp.where((quadrant & 2) != 0, -second, second),
    )


def mod_phase(first, second):
    return (first * second) & (NTOT - 1)


def split(facets):
    groups = max(1, facets // TILE)
    inside = TILE * groups // facets
    return groups, S // TILE // groups, inside


def along_kernel(facets, cols, chunk, scal, offsets, names, strip, out, held, table, total, outside, small, sems):
    count = held.shape[1]
    steps = count // chunk
    slots = names.shape[2]
    copies = {}
    notes = []
    for n, (src, dst) in enumerate(zip((offsets, names), small)):
        notes.append(pltpu.make_async_copy(src, dst, sems.at[steps + n]))
        notes[n].start()
    for n in reversed(range(steps)):
        part = pl.ds(n * chunk, chunk)
        copies[n] = pltpu.make_async_copy(strip.at[:, part], held.at[:, part], sems.at[n])
        copies[n].start()
    row_start = scal[0]
    rows = S // facets
    groups, tall, inside = split(facets)

    def sample_of(place):
        owner = place // rows
        within = place % rows
        group = owner // (facets // groups)
        line = (owner % (facets // groups)) * inside + within // tall
        return (within % tall + tall * group) * TILE + line

    blocks = S // 8
    inner = row_start + (NTOT // L) * sample_of(lax.broadcasted_iota(I32, (8, W), 0))
    outer = (NTOT // L) * sample_of(8 * lax.broadcasted_iota(I32, (blocks, W), 0))
    factors = {}

    def factor_tables(n, column, wide_column, scale):
        cosine, sine = cos_sin(mod_phase(inner, column))
        factors[n] = (cosine * scale, sine * scale)
        cosine, sine = cos_sin(mod_phase(outer, wide_column))
        outside[2 * n] = cosine
        outside[2 * n + 1] = sine

    def factor(n, k):
        cosine, sine = outside[2 * n, k : k + 1, :], outside[2 * n + 1, k : k + 1, :]
        x, y = factors[n]
        return x * cosine - y * sine, y * cosine + x * sine

    factor_tables(
        0,
        lax.broadcasted_iota(I32, (8, W), 1),
        lax.broadcasted_iota(I32, (blocks, W), 1),
        1.0 / math.sqrt(L),
    )
    factor_tables(1, W, W, 1.0)
    factor_tables(2, chunk, chunk, 1.0)
    for k in range(blocks):
        c1, s1 = factor(0, k)
        turn_c, turn_s = factor(1, k)
        twice = turn_c + turn_c
        for local in range(chunk // W):
            if local == 1:
                c0, s0 = c1, s1
                c1, s1 = c0 * turn_c - s0 * turn_s, s0 * turn_c + c0 * turn_s
            elif local:
                c0, c1 = c1, twice * c1 - c0
                s0, s1 = s1, twice * s1 - s0
            at = slice(local * W, (local + 1) * W)
            table[8 * k : 8 * k + 8, at] = c1.astype(BF16)
            table[S + 8 * k : S + 8 * k + 8, at] = s1.astype(BF16)
    for n in reversed(range(steps)):
        copies[n].wait()
        if n == 0:
            notes[0].wait()
            col_start = small[0][0, 0] + lax.axis_index("col") * count
            factor_tables(3, col_start, col_start, 1.0)
        part = slice(n * chunk, (n + 1) * chunk)
        cells = jnp.concatenate([held[0, part, :], held[1, part, :]], axis=1)
        upper = jnp.dot(table[0:S, :], cells, preferred_element_type=F32)
        lower = jnp.dot(table[S : 2 * S, :], cells, preferred_element_type=F32)
        for k in range(blocks):
            at = slice(8 * k, 8 * k + 8)
            re = upper[at, 0:W] + lower[at, W : 2 * W]
            im = upper[at, W : 2 * W] - lower[at, 0:W]
            if n + 1 < steps:
                old_re, old_im = total[at, 0:W], total[at, W : 2 * W]
                leap_c, leap_s = factor(2, k)
                re = re + (old_re * leap_c + old_im * leap_s)
                im = im + (old_im * leap_c - old_re * leap_s)
            if n == 0:
                turn_c, turn_s = factor(3, k)
                re, im = re * turn_c + im * turn_s, im * turn_c - re * turn_s
            total[at, 0:W] = re
            total[at, W : 2 * W] = im
    notes[1].wait()
    across = small[0][0, 1]
    spot = lax.broadcasted_iota(I32, (2, W), 1)
    note = jnp.where(spot == W - 2, across >> 8, jnp.where(spot == W - 1, across & 255, 0))
    for j in range(slots):
        note = jnp.where(spot == j, small[1][0, 0, j], note)
    note = note.astype(F32).astype(BF16)
    for o in range(facets):
        re = total[o * rows : (o + 1) * rows, 0:W].astype(BF16)
        im = total[o * rows : (o + 1) * rows, W : 2 * W].astype(BF16)
        for c in range(cols):
            at = (o * cols + c) * (2 * rows + 2)
            out[at : at + rows, :] = re
            out[at + rows : at + 2 * rows, :] = im
            out[at + 2 * rows : at + 2 * rows + 2, :] = note


def along(strip, row_offsets, facet_offsets, names, facets, cols):
    count = strip.shape[1]
    chunk = min(CHUNK, count)
    rows = S // facets
    return pl.pallas_call(
        functools.partial(along_kernel, facets, cols, chunk),
        out_shape=jax.ShapeDtypeStruct((facets * cols * (2 * rows + 2), W), BF16),
        in_specs=[pl.BlockSpec(memory_space=pltpu.SMEM)]
        + [pl.BlockSpec(memory_space=pltpu.HBM)] * 3,
        out_specs=pl.BlockSpec(memory_space=pltpu.VMEM),
        scratch_shapes=[
            pltpu.VMEM((2, count, W), BF16),
            pltpu.VMEM((2 * S, chunk), BF16),
            pltpu.VMEM((S, 2 * W), F32),
            pltpu.VMEM((8, S // 8, W), F32),
            [
                pltpu.SMEM(facet_offsets.shape, I32),
                pltpu.SMEM(names.shape, I32),
            ],
            pltpu.SemaphoreType.DMA((count // chunk + 2,)),
        ],
        cost_estimate=pl.CostEstimate(
            flops=8 * S * W * count, bytes_accessed=4 * count * W, transcendentals=0
        ),
        name="along",
    )(row_offsets, facet_offsets, names, strip)


def base_kernel(columns, out):
    cell = lax.broadcasted_iota(I32, (W, 2 * S), 0)
    lane = lax.broadcasted_iota(I32, (W, 2 * S), 1)
    turn = ((lane >> 5) & 1) * (NTOT // 4)
    top, bottom = cos_sin((cell * positions(columns[0], lane) + turn) & (NTOT - 1))
    scale = 1.0 / math.sqrt(W)
    out[0:W, :] = (top * scale).astype(BF16)
    out[W : 2 * W, :] = (bottom * scale).astype(BF16)


def positions(column, lane):
    return column + (NTOT // S) * ((lane >> 6) * TILE + (lane & (TILE - 1)))


def base(columns):
    return pl.pallas_call(
        base_kernel,
        out_shape=jax.ShapeDtypeStruct((2 * W, 2 * S), BF16),
        in_specs=[pl.BlockSpec(memory_space=pltpu.SMEM)],
        out_specs=pl.BlockSpec(memory_space=pltpu.VMEM),
        compiler_params=pltpu.CompilerParams(vmem_limit_bytes=VMEM_LIMIT),
        cost_estimate=pl.CostEstimate(flops=1 << 24, bytes_accessed=1 << 18, transcendentals=0),
        name="base",
    )(columns)


def across_kernel(facets, cols, columns, got, right, out, left, summed, phases):
    rows = S // facets
    groups, tall, inside = split(facets)
    slots = out.shape[1]
    wide = 2 * S
    height = facets * rows
    size = 2 * rows + 2
    column = lax.axis_index("col")
    sources = []
    for f in range(facets):
        parts = []
        for part in range(2):
            at = f * cols * size + part * rows
            value = got[at : at + rows, :].astype(F32)
            for h in range(1, cols):
                value = value + got[at + h * size : at + h * size + rows, :].astype(F32)
            parts.append(value)
        re, im = parts
        left[f * rows : (f + 1) * rows, 0:W] = re
        left[f * rows : (f + 1) * rows, W : 2 * W] = im
        left[height + f * rows : height + (f + 1) * rows, 0:W] = im
        left[height + f * rows : height + (f + 1) * rows, W : 2 * W] = -re
        note = None
        for h in range(cols):
            at = (f * cols + h) * size + 2 * rows
            value = jnp.where(column == h, got[at : at + 2, :].astype(F32)[0:1], 0.0)
            note = value if note is None else note + value
        sources.append(note)
    summed[...] = jnp.dot(left[...].astype(BF16), right[...], preferred_element_type=F32)
    heads = jnp.concatenate(sources, axis=0)
    offset = (heads[:, W - 2 : W - 1] * 256.0 + heads[:, W - 1 : W]).astype(I32)
    lane = lax.broadcasted_iota(I32, (facets, wide), 1)
    cosine, sine = cos_sin(mod_phase(offset, positions(columns[0], lane)))
    phases[0] = cosine
    phases[1] = sine
    acc = jnp.zeros((rows, wide), F32)
    for f in range(facets):
        acc = acc + summed[f * rows : (f + 1) * rows, :] * phases[0, f : f + 1, :]
        acc = acc + summed[height + f * rows : height + (f + 1) * rows, :] * phases[1, f : f + 1, :]
    acc = acc * (1.0 / math.sqrt(facets))
    pieces = []
    for b in range(S // TILE):
        at = slice(b * 2 * TILE, (b + 1) * 2 * TILE)
        parts = [acc[i * tall : (i + 1) * tall, at] for i in range(inside)]
        if inside == 1:
            parts.append(jnp.zeros_like(parts[0]))
        pieces.append(jnp.concatenate(parts, axis=1))
    tiles = jnp.concatenate(pieces, axis=0).astype(BF16)
    line = lax.broadcasted_iota(I32, (facets * slots, facets), 0)
    place = line - slots * lax.broadcasted_iota(I32, line.shape, 1)
    owner = jnp.where((place >= 0) & (place < slots), 1.0, 0.0)
    spread = jnp.dot(owner.astype(BF16), heads.astype(BF16), preferred_element_type=F32)
    line = lax.broadcasted_iota(I32, spread.shape, 0)
    own = lax.broadcasted_iota(I32, spread.shape, 1) == (line & (slots - 1))
    names = jnp.sum(jnp.where(own, spread, 0.0), axis=1, keepdims=True).astype(I32)
    first = (lax.axis_index("facet") // (facets // groups)) * tall
    local = (names >> 3) - first
    wanted = jnp.where((local >= 0) & (local < tall), (names & 7) * tall + local, -1)
    count = tiles.shape[0]
    spot = lax.broadcasted_iota(I32, (facets * slots, W), 1)
    onehot = jnp.where(wanted == spot, 1.0, 0.0).astype(BF16)[:, 0:count]
    chosen = jnp.dot(onehot, tiles, preferred_element_type=F32)
    for o in range(facets):
        out[o] = chosen[o * slots : (o + 1) * slots, :].astype(BF16)


def across(got, right, columns, slots, facets, cols):
    return pl.pallas_call(
        functools.partial(across_kernel, facets, cols),
        out_shape=jax.ShapeDtypeStruct((facets, slots, W), BF16),
        in_specs=[
            pl.BlockSpec(memory_space=pltpu.SMEM),
            pl.BlockSpec(memory_space=pltpu.VMEM),
            pl.BlockSpec(memory_space=pltpu.VMEM),
        ],
        out_specs=pl.BlockSpec(memory_space=pltpu.VMEM),
        scratch_shapes=[
            pltpu.VMEM((2 * S, 2 * W), F32),
            pltpu.VMEM((2 * S, 2 * S), F32),
            pltpu.VMEM((2, facets, 2 * S), F32),
        ],
        compiler_params=pltpu.CompilerParams(vmem_limit_bytes=VMEM_LIMIT),
        cost_estimate=pl.CostEstimate(
            flops=2 * 2 * S * 2 * W * 2 * S, bytes_accessed=1 << 20, transcendentals=0
        ),
        name="across",
    )(columns, got, right)


def waves_kernel(facets, live, uv, right, near, far):
    _, _, inside = split(facets)
    vis = uv.shape[2]
    step = NTOT // UV_STEPS
    line = lax.broadcasted_iota(I32, (TILE, vis), 0)
    low = line[0:8] * inside
    high = (line[0:4] % (4 // inside)) * 8 * inside + line[0:4] // (4 // inside)

    def slot(j, carry):
        cosine, sine = cos_sin((uv[j, 1:2, :] * (line * step)) & (NTOT - 1))
        cos_high, sin_high = cosine.astype(BF16), sine.astype(BF16)
        right[j, 0:TILE, :] = cos_high
        right[j, TILE : 2 * TILE, :] = sin_high
        right[j, 2 * TILE : 3 * TILE, :] = (cosine - cos_high.astype(F32)).astype(BF16)
        right[j, 3 * TILE : 4 * TILE, :] = (sine - sin_high.astype(F32)).astype(BF16)
        cosine, sine = cos_sin((uv[j, 0:1, :] * (low * step)) & (NTOT - 1))
        size = jnp.where(j < live[0, 0], 1.0 / TILE, 0.0)
        near[j, 0] = cosine * size
        near[j, 1] = sine * size
        cosine, sine = cos_sin((uv[j, 0:1, :] * (high * step)) & (NTOT - 1))
        far[j, 0] = cosine
        far[j, 1] = sine
        return carry

    lax.fori_loop(0, uv.shape[0], slot, 0)


def waves(live, uv, facets):
    slots, _, vis = uv.shape
    return pl.pallas_call(
        functools.partial(waves_kernel, facets),
        out_shape=(
            jax.ShapeDtypeStruct((slots, 4 * TILE, vis), BF16),
            jax.ShapeDtypeStruct((slots, 2, 8, vis), F32),
            jax.ShapeDtypeStruct((slots, 2, 4, vis), F32),
        ),
        in_specs=[
            pl.BlockSpec(memory_space=pltpu.SMEM),
            pl.BlockSpec(memory_space=pltpu.VMEM),
        ],
        out_specs=[pl.BlockSpec(memory_space=pltpu.VMEM)] * 3,
        compiler_params=pltpu.CompilerParams(vmem_limit_bytes=VMEM_LIMIT),
        cost_estimate=pl.CostEstimate(flops=1 << 26, bytes_accessed=3 << 20, transcendentals=0),
        name="waves",
    )(live, uv)


def visibility_kernel(facets, parts, right, near, far, out, held):
    groups, _, inside = split(facets)
    slots = out.shape[0]
    sources = facets // groups
    for f in range(sources):
        held[f] = parts[f].astype(F32)
        for g in range(1, groups):
            held[f] += parts[g * sources + f].astype(F32)
    lane = lax.broadcasted_iota(I32, (sources, W), 1)
    sign = jnp.where((lane & TILE) == 0, 1.0, -1.0).astype(F32)
    for j in range(slots):
        x = held[:, j, :]
        y = pltpu.roll(x, W // 2, 1)
        both = [jnp.where(lane < W // 2, x, y), jnp.where(lane < W // 2, y, x)][:inside]
        lhs = [z * sign for z in both] + [pltpu.roll(z, TILE, 1) for z in both]
        middle = jnp.dot(
            jnp.concatenate(lhs, axis=0).astype(BF16), right[j], preferred_element_type=F32
        )
        real, imag = middle[0:8], middle[TILE : TILE + 8]
        for h in range(1, 4):
            more_re = middle[8 * h : 8 * h + 8]
            more_im = middle[TILE + 8 * h : TILE + 8 * h + 8]
            cosine, sine = far[j, 0, h : h + 1, :], far[j, 1, h : h + 1, :]
            real = real + (cosine * more_re - sine * more_im)
            imag = imag + (cosine * more_im + sine * more_re)
        cosine, sine = near[j, 0], near[j, 1]
        out[j, 0:1, :] = jnp.sum(cosine * real - sine * imag, axis=0, keepdims=True)
        out[j, 1:2, :] = jnp.sum(cosine * imag + sine * real, axis=0, keepdims=True)


def visibilities_of(parts, tables, facets):
    slots, _, vis = tables[0].shape
    return pl.pallas_call(
        functools.partial(visibility_kernel, facets),
        out_shape=jax.ShapeDtypeStruct((slots, 2, vis), F32),
        in_specs=[pl.BlockSpec(memory_space=pltpu.VMEM)] * 4,
        out_specs=pl.BlockSpec(memory_space=pltpu.VMEM),
        scratch_shapes=[pltpu.VMEM((facets // split(facets)[0], slots, W), F32)],
        compiler_params=pltpu.CompilerParams(vmem_limit_bytes=VMEM_LIMIT),
        cost_estimate=pl.CostEstimate(
            flops=slots * 2 * 64 * 128 * vis, bytes_accessed=1 << 20, transcendentals=0
        ),
        name="visibility",
    )(parts, *tables)


def shards(
    facet_strips, facet_offsets, column_offsets, row_offsets, tile_lists, tile_counts, uv_index
):
    facets, cols = lax.axis_size("facet"), lax.axis_size("col")
    sent = along(facet_strips[0], row_offsets, facet_offsets, tile_lists, facets, cols)
    pairs = sent.reshape((facets * cols, -1, 2, W))
    got = lax.all_to_all(pairs, ("facet", "col"), 0, 0, tiled=True)
    got = got.reshape(sent.shape)
    right = base(column_offsets)
    tables = waves(tile_counts, uv_index[0, 0], facets)
    asked = across(got, right, column_offsets, tile_lists.shape[2], facets, cols)
    parts = lax.all_to_all(asked, "facet", 0, 0, tiled=True)
    result = visibilities_of(parts, tables, facets)
    return result[None, None]


def solution(mesh):
    in_specs = (
        P("facet", None, "col", None),
        P("facet", None),
        P("col"),
        P(),
        P("col", "facet", None),
        P("col", "facet"),
        P("col", "facet", None, None, None),
    )
    out_specs = P("col", "facet", None, None, None)
    return jax.shard_map(shards, mesh=mesh, in_specs=in_specs, out_specs=out_specs, check_vma=False)
```

```python
import functools
import math

import jax
import jax.numpy as jnp
from jax import lax
from jax.experimental import pallas as pl
from jax.experimental.pallas import tpu as pltpu
from jax.sharding import PartitionSpec as P


L = 8192
W = 128
S = 256
TILE = 32
NTOT = 65536
UV_STEPS = 4096
VMEM_LIMIT = 16 << 20
CHUNK = 2048
BF16 = jnp.bfloat16
F32 = jnp.float32
I32 = jnp.int32


def cos_sin(index):
    shifted = index + NTOT // 8
    quadrant = shifted >> 14
    rest = (shifted & (NTOT // 4 - 1)) - NTOT // 8
    x = rest.astype(F32) * (2.0 * math.pi / NTOT)
    y = x * x
    sine = x + x * (y * (-1.0 / 6 + y * (1.0 / 120 + y * (-1.0 / 5040 + y * (1.0 / 362880)))))
    cosine = 1.0 + y * (-0.5 + y * (1.0 / 24 + y * (-1.0 / 720 + y * (1.0 / 40320))))
    odd = (quadrant & 1) != 0
    first = jnp.where(odd, sine, cosine)
    second = jnp.where(odd, cosine, sine)
    return (
        jnp.where(((quadrant + 1) & 2) != 0, -first, first),
        jnp.where((quadrant & 2) != 0, -second, second),
    )


def mod_phase(first, second):
    return (first * second) & (NTOT - 1)


def split(facets):
    groups = max(1, facets // TILE)
    inside = TILE * groups // facets
    return groups, S // TILE // groups, inside


def along_kernel(facets, cols, chunk, scal, offsets, names, strip, out, held, table, total, outside, small, sems):
    count = held.shape[1]
    steps = count // chunk
    slots = names.shape[2]
    copies = {}
    notes = []
    for n, (src, dst) in enumerate(zip((offsets, names), small)):
        notes.append(pltpu.make_async_copy(src, dst, sems.at[steps + n]))
        notes[n].start()
    for n in reversed(range(steps)):
        part = pl.ds(n * chunk, chunk)
        copies[n] = pltpu.make_async_copy(strip.at[:, part], held.at[:, part], sems.at[n])
        copies[n].start()
    row_start = scal[0]
    rows = S // facets
    groups, tall, inside = split(facets)

    def sample_of(place):
        owner = place // rows
        within = place % rows
        group = owner // (facets // groups)
        line = (owner % (facets // groups)) * inside + within // tall
        return (within % tall + tall * group) * TILE + line

    blocks = S // 8
    inner = row_start + (NTOT // L) * sample_of(lax.broadcasted_iota(I32, (8, W), 0))
    outer = (NTOT // L) * sample_of(8 * lax.broadcasted_iota(I32, (blocks, W), 0))
    factors = {}

    def factor_tables(n, column, wide_column, scale):
        cosine, sine = cos_sin(mod_phase(inner, column))
        factors[n] = (cosine * scale, sine * scale)
        cosine, sine = cos_sin(mod_phase(outer, wide_column))
        outside[2 * n] = cosine
        outside[2 * n + 1] = sine

    def factor(n, k):
        cosine, sine = outside[2 * n, k : k + 1, :], outside[2 * n + 1, k : k + 1, :]
        x, y = factors[n]
        return x * cosine - y * sine, y * cosine + x * sine

    factor_tables(
        0,
        lax.broadcasted_iota(I32, (8, W), 1),
        lax.broadcasted_iota(I32, (blocks, W), 1),
        1.0 / math.sqrt(L),
    )
    factor_tables(1, W, W, 1.0)
    factor_tables(2, chunk, chunk, 1.0)
    for k in range(blocks):
        c1, s1 = factor(0, k)
        turn_c, turn_s = factor(1, k)
        twice = turn_c + turn_c
        for local in range(chunk // W):
            if local == 1:
                c0, s0 = c1, s1
                c1, s1 = c0 * turn_c - s0 * turn_s, s0 * turn_c + c0 * turn_s
            elif local:
                c0, c1 = c1, twice * c1 - c0
                s0, s1 = s1, twice * s1 - s0
            at = slice(local * W, (local + 1) * W)
            table[8 * k : 8 * k + 8, at] = c1.astype(BF16)
            table[S + 8 * k : S + 8 * k + 8, at] = s1.astype(BF16)
    for n in reversed(range(steps)):
        copies[n].wait()
        if n == 0:
            notes[0].wait()
            col_start = small[0][0, 0] + lax.axis_index("col") * count
            factor_tables(3, col_start, col_start, 1.0)
        part = slice(n * chunk, (n + 1) * chunk)
        cells = jnp.concatenate([held[0, part, :], held[1, part, :]], axis=1)
        upper = jnp.dot(table[0:S, :], cells, preferred_element_type=F32)
        lower = jnp.dot(table[S : 2 * S, :], cells, preferred_element_type=F32)
        for k in range(blocks):
            at = slice(8 * k, 8 * k + 8)
            re = upper[at, 0:W] + lower[at, W : 2 * W]
            im = upper[at, W : 2 * W] - lower[at, 0:W]
            if n + 1 < steps:
                old_re, old_im = total[at, 0:W], total[at, W : 2 * W]
                leap_c, leap_s = factor(2, k)
                re = re + (old_re * leap_c + old_im * leap_s)
                im = im + (old_im * leap_c - old_re * leap_s)
            if n == 0:
                turn_c, turn_s = factor(3, k)
                re, im = re * turn_c + im * turn_s, im * turn_c - re * turn_s
            total[at, 0:W] = re
            total[at, W : 2 * W] = im
    notes[1].wait()
    across = small[0][0, 1]
    spot = lax.broadcasted_iota(I32, (2, W), 1)
    note = jnp.where(spot == W - 2, across >> 8, jnp.where(spot == W - 1, across & 255, 0))
    for j in range(slots):
        note = jnp.where(spot == j, small[1][0, 0, j], note)
    note = note.astype(F32).astype(BF16)
    for o in range(facets):
        re = total[o * rows : (o + 1) * rows, 0:W].astype(BF16)
        im = total[o * rows : (o + 1) * rows, W : 2 * W].astype(BF16)
        for c in range(cols):
            at = (o * cols + c) * (2 * rows + 2)
            out[at : at + rows, :] = re
            out[at + rows : at + 2 * rows, :] = im
            out[at + 2 * rows : at + 2 * rows + 2, :] = note


def along(strip, row_offsets, facet_offsets, names, facets, cols):
    count = strip.shape[1]
    chunk = min(CHUNK, count)
    rows = S // facets
    return pl.pallas_call(
        functools.partial(along_kernel, facets, cols, chunk),
        out_shape=jax.ShapeDtypeStruct((facets * cols * (2 * rows + 2), W), BF16),
        in_specs=[pl.BlockSpec(memory_space=pltpu.SMEM)]
        + [pl.BlockSpec(memory_space=pltpu.HBM)] * 3,
        out_specs=pl.BlockSpec(memory_space=pltpu.VMEM),
        scratch_shapes=[
            pltpu.VMEM((2, count, W), BF16),
            pltpu.VMEM((2 * S, chunk), BF16),
            pltpu.VMEM((S, 2 * W), F32),
            pltpu.VMEM((8, S // 8, W), F32),
            [
                pltpu.SMEM(facet_offsets.shape, I32),
                pltpu.SMEM(names.shape, I32),
            ],
            pltpu.SemaphoreType.DMA((count // chunk + 2,)),
        ],
        cost_estimate=pl.CostEstimate(
            flops=8 * S * W * count, bytes_accessed=4 * count * W, transcendentals=0
        ),
        name="along",
    )(row_offsets, facet_offsets, names, strip)


def base_kernel(columns, out):
    cell = lax.broadcasted_iota(I32, (W, 2 * S), 0)
    lane = lax.broadcasted_iota(I32, (W, 2 * S), 1)
    turn = ((lane >> 5) & 1) * (NTOT // 4)
    top, bottom = cos_sin((cell * positions(columns[0], lane) + turn) & (NTOT - 1))
    scale = 1.0 / math.sqrt(W)
    out[0:W, :] = (top * scale).astype(BF16)
    out[W : 2 * W, :] = (bottom * scale).astype(BF16)


def positions(column, lane):
    return column + (NTOT // S) * ((lane >> 6) * TILE + (lane & (TILE - 1)))


def base(columns):
    return pl.pallas_call(
        base_kernel,
        out_shape=jax.ShapeDtypeStruct((2 * W, 2 * S), BF16),
        in_specs=[pl.BlockSpec(memory_space=pltpu.SMEM)],
        out_specs=pl.BlockSpec(memory_space=pltpu.VMEM),
        compiler_params=pltpu.CompilerParams(vmem_limit_bytes=VMEM_LIMIT),
        cost_estimate=pl.CostEstimate(flops=1 << 24, bytes_accessed=1 << 18, transcendentals=0),
        name="base",
    )(columns)


def across_kernel(facets, cols, columns, got, right, out, left, summed, phases):
    rows = S // facets
    groups, tall, inside = split(facets)
    slots = out.shape[1]
    wide = 2 * S
    height = facets * rows
    size = 2 * rows + 2
    column = lax.axis_index("col")
    sources = []
    for f in range(facets):
        for h in range(cols):
            at = (f * cols + h) * size
            re, im = got[at : at + rows, :], got[at + rows : at + 2 * rows, :]
            near, far = slice(2 * h * W, (2 * h + 1) * W), slice((2 * h + 1) * W, (2 * h + 2) * W)
            left[f * rows : (f + 1) * rows, near] = re
            left[f * rows : (f + 1) * rows, far] = im
            left[height + f * rows : height + (f + 1) * rows, near] = im
            left[height + f * rows : height + (f + 1) * rows, far] = -re
        note = None
        for h in range(cols):
            at = (f * cols + h) * size + 2 * rows
            value = jnp.where(column == h, got[at : at + 2, :].astype(F32)[0:1], 0.0)
            note = value if note is None else note + value
        sources.append(note)
    table = jnp.concatenate([right[...]] * cols, axis=0)
    summed[...] = jnp.dot(left[...], table, preferred_element_type=F32)
    heads = jnp.concatenate(sources, axis=0)
    offset = (heads[:, W - 2 : W - 1] * 256.0 + heads[:, W - 1 : W]).astype(I32)
    lane = lax.broadcasted_iota(I32, (facets, wide), 1)
    cosine, sine = cos_sin(mod_phase(offset, positions(columns[0], lane)))
    phases[0] = cosine
    phases[1] = sine
    acc = jnp.zeros((rows, wide), F32)
    for f in range(facets):
        acc = acc + summed[f * rows : (f + 1) * rows, :] * phases[0, f : f + 1, :]
        acc = acc + summed[height + f * rows : height + (f + 1) * rows, :] * phases[1, f : f + 1, :]
    acc = acc * (1.0 / math.sqrt(facets))
    pieces = []
    for b in range(S // TILE):
        at = slice(b * 2 * TILE, (b + 1) * 2 * TILE)
        parts = [acc[i * tall : (i + 1) * tall, at] for i in range(inside)]
        if inside == 1:
            parts.append(jnp.zeros_like(parts[0]))
        pieces.append(jnp.concatenate(parts, axis=1))
    tiles = jnp.concatenate(pieces, axis=0).astype(BF16)
    line = lax.broadcasted_iota(I32, (facets * slots, facets), 0)
    place = line - slots * lax.broadcasted_iota(I32, line.shape, 1)
    owner = jnp.where((place >= 0) & (place < slots), 1.0, 0.0)
    spread = jnp.dot(owner.astype(BF16), heads.astype(BF16), preferred_element_type=F32)
    line = lax.broadcasted_iota(I32, spread.shape, 0)
    own = lax.broadcasted_iota(I32, spread.shape, 1) == (line & (slots - 1))
    names = jnp.sum(jnp.where(own, spread, 0.0), axis=1, keepdims=True).astype(I32)
    first = (lax.axis_index("facet") // (facets // groups)) * tall
    local = (names >> 3) - first
    wanted = jnp.where((local >= 0) & (local < tall), (names & 7) * tall + local, -1)
    count = tiles.shape[0]
    spot = lax.broadcasted_iota(I32, (facets * slots, W), 1)
    onehot = jnp.where(wanted == spot, 1.0, 0.0).astype(BF16)[:, 0:count]
    chosen = jnp.dot(onehot, tiles, preferred_element_type=F32)
    for o in range(facets):
        out[o] = chosen[o * slots : (o + 1) * slots, :].astype(BF16)


def across(got, right, columns, slots, facets, cols):
    return pl.pallas_call(
        functools.partial(across_kernel, facets, cols),
        out_shape=jax.ShapeDtypeStruct((facets, slots, W), BF16),
        in_specs=[
            pl.BlockSpec(memory_space=pltpu.SMEM),
            pl.BlockSpec(memory_space=pltpu.VMEM),
            pl.BlockSpec(memory_space=pltpu.VMEM),
        ],
        out_specs=pl.BlockSpec(memory_space=pltpu.VMEM),
        scratch_shapes=[
            pltpu.VMEM((2 * S, 2 * W * cols), BF16),
            pltpu.VMEM((2 * S, 2 * S), F32),
            pltpu.VMEM((2, facets, 2 * S), F32),
        ],
        compiler_params=pltpu.CompilerParams(vmem_limit_bytes=VMEM_LIMIT),
        cost_estimate=pl.CostEstimate(
            flops=2 * 2 * S * 2 * W * 2 * S, bytes_accessed=1 << 20, transcendentals=0
        ),
        name="across",
    )(columns, got, right)


def waves_kernel(facets, live, uv, right, near, far):
    _, _, inside = split(facets)
    vis = uv.shape[2]
    step = NTOT // UV_STEPS
    line = lax.broadcasted_iota(I32, (TILE, vis), 0)
    low = line[0:8] * inside
    high = (line[0:4] % (4 // inside)) * 8 * inside + line[0:4] // (4 // inside)

    def slot(j, carry):
        cosine, sine = cos_sin((uv[j, 1:2, :] * (line * step)) & (NTOT - 1))
        cos_high, sin_high = cosine.astype(BF16), sine.astype(BF16)
        right[j, 0:TILE, :] = cos_high
        right[j, TILE : 2 * TILE, :] = sin_high
        right[j, 2 * TILE : 3 * TILE, :] = (cosine - cos_high.astype(F32)).astype(BF16)
        right[j, 3 * TILE : 4 * TILE, :] = (sine - sin_high.astype(F32)).astype(BF16)
        cosine, sine = cos_sin((uv[j, 0:1, :] * (low * step)) & (NTOT - 1))
        size = jnp.where(j < live[0, 0], 1.0 / TILE, 0.0)
        near[j, 0] = cosine * size
        near[j, 1] = sine * size
        cosine, sine = cos_sin((uv[j, 0:1, :] * (high * step)) & (NTOT - 1))
        far[j, 0] = cosine
        far[j, 1] = sine
        return carry

    lax.fori_loop(0, uv.shape[0], slot, 0)


def waves(live, uv, facets):
    slots, _, vis = uv.shape
    return pl.pallas_call(
        functools.partial(waves_kernel, facets),
        out_shape=(
            jax.ShapeDtypeStruct((slots, 4 * TILE, vis), BF16),
            jax.ShapeDtypeStruct((slots, 2, 8, vis), F32),
            jax.ShapeDtypeStruct((slots, 2, 4, vis), F32),
        ),
        in_specs=[
            pl.BlockSpec(memory_space=pltpu.SMEM),
            pl.BlockSpec(memory_space=pltpu.VMEM),
        ],
        out_specs=[pl.BlockSpec(memory_space=pltpu.VMEM)] * 3,
        compiler_params=pltpu.CompilerParams(vmem_limit_bytes=VMEM_LIMIT),
        cost_estimate=pl.CostEstimate(flops=1 << 26, bytes_accessed=3 << 20, transcendentals=0),
        name="waves",
    )(live, uv)


def visibility_kernel(facets, parts, right, near, far, out, held):
    groups, _, inside = split(facets)
    slots = out.shape[0]
    sources = facets // groups
    for f in range(sources):
        held[f] = parts[f].astype(F32)
        for g in range(1, groups):
            held[f] += parts[g * sources + f].astype(F32)
    lane = lax.broadcasted_iota(I32, (sources, W), 1)
    sign = jnp.where((lane & TILE) == 0, 1.0, -1.0).astype(F32)
    for j in range(slots):
        x = held[:, j, :]
        y = pltpu.roll(x, W // 2, 1)
        both = [jnp.where(lane < W // 2, x, y), jnp.where(lane < W // 2, y, x)][:inside]
        lhs = [z * sign for z in both] + [pltpu.roll(z, TILE, 1) for z in both]
        middle = jnp.dot(
            jnp.concatenate(lhs, axis=0).astype(BF16), right[j], preferred_element_type=F32
        )
        real, imag = middle[0:8], middle[TILE : TILE + 8]
        for h in range(1, 4):
            more_re = middle[8 * h : 8 * h + 8]
            more_im = middle[TILE + 8 * h : TILE + 8 * h + 8]
            cosine, sine = far[j, 0, h : h + 1, :], far[j, 1, h : h + 1, :]
            real = real + (cosine * more_re - sine * more_im)
            imag = imag + (cosine * more_im + sine * more_re)
        cosine, sine = near[j, 0], near[j, 1]
        out[j, 0:1, :] = jnp.sum(cosine * real - sine * imag, axis=0, keepdims=True)
        out[j, 1:2, :] = jnp.sum(cosine * imag + sine * real, axis=0, keepdims=True)


def visibilities_of(parts, tables, facets):
    slots, _, vis = tables[0].shape
    return pl.pallas_call(
        functools.partial(visibility_kernel, facets),
        out_shape=jax.ShapeDtypeStruct((slots, 2, vis), F32),
        in_specs=[pl.BlockSpec(memory_space=pltpu.VMEM)] * 4,
        out_specs=pl.BlockSpec(memory_space=pltpu.VMEM),
        scratch_shapes=[pltpu.VMEM((facets // split(facets)[0], slots, W), F32)],
        compiler_params=pltpu.CompilerParams(vmem_limit_bytes=VMEM_LIMIT),
        cost_estimate=pl.CostEstimate(
            flops=slots * 2 * 64 * 128 * vis, bytes_accessed=1 << 20, transcendentals=0
        ),
        name="visibility",
    )(parts, *tables)


def shards(
    facet_strips, facet_offsets, column_offsets, row_offsets, tile_lists, tile_counts, uv_index
):
    facets, cols = lax.axis_size("facet"), lax.axis_size("col")
    sent = along(facet_strips[0], row_offsets, facet_offsets, tile_lists, facets, cols)
    pairs = sent.reshape((facets * cols, -1, 2, W))
    got = lax.all_to_all(pairs, ("facet", "col"), 0, 0, tiled=True)
    got = got.reshape(sent.shape)
    right = base(column_offsets)
    tables = waves(tile_counts, uv_index[0, 0], facets)
    asked = across(got, right, column_offsets, tile_lists.shape[2], facets, cols)
    parts = lax.all_to_all(asked, "facet", 0, 0, tiled=True)
    result = visibilities_of(parts, tables, facets)
    return result[None, None]


def solution(mesh):
    in_specs = (
        P("facet", None, "col", None),
        P("facet", None),
        P("col"),
        P(),
        P("col", "facet", None),
        P("col", "facet"),
        P("col", "facet", None, None, None),
    )
    out_specs = P("col", "facet", None, None, None)
    return jax.shard_map(shards, mesh=mesh, in_specs=in_specs, out_specs=out_specs, check_vma=False)
```

```python
import functools
import math

import jax
import jax.numpy as jnp
from jax import lax
from jax.experimental import pallas as pl
from jax.experimental.pallas import tpu as pltpu
from jax.sharding import PartitionSpec as P


L = 8192
W = 128
S = 256
TILE = 32
NTOT = 65536
UV_STEPS = 4096
VMEM_LIMIT = 16 << 20
CHUNK = 2048
BF16 = jnp.bfloat16
F32 = jnp.float32
I32 = jnp.int32


def cos_sin(index):
    shifted = index + NTOT // 8
    quadrant = shifted >> 14
    rest = (shifted & (NTOT // 4 - 1)) - NTOT // 8
    x = rest.astype(F32) * (2.0 * math.pi / NTOT)
    y = x * x
    sine = x + x * (y * (-1.0 / 6 + y * (1.0 / 120 + y * (-1.0 / 5040 + y * (1.0 / 362880)))))
    cosine = 1.0 + y * (-0.5 + y * (1.0 / 24 + y * (-1.0 / 720 + y * (1.0 / 40320))))
    odd = (quadrant & 1) != 0
    first = jnp.where(odd, sine, cosine)
    second = jnp.where(odd, cosine, sine)
    return (
        jnp.where(((quadrant + 1) & 2) != 0, -first, first),
        jnp.where((quadrant & 2) != 0, -second, second),
    )


def mod_phase(first, second):
    return (first * second) & (NTOT - 1)


def split(facets):
    groups = max(1, facets // TILE)
    inside = TILE * groups // facets
    return groups, S // TILE // groups, inside


def along_kernel(facets, cols, chunk, scal, offsets, names, strip, out, held, table, total, outside, small, sems):
    count = held.shape[1]
    steps = count // chunk
    slots = names.shape[2]
    copies = {}
    notes = []
    for n, (src, dst) in enumerate(zip((offsets, names), small)):
        notes.append(pltpu.make_async_copy(src, dst, sems.at[steps + n]))
        notes[n].start()
    for n in reversed(range(steps)):
        part = pl.ds(n * chunk, chunk)
        copies[n] = pltpu.make_async_copy(strip.at[:, part], held.at[:, part], sems.at[n])
        copies[n].start()
    row_start = scal[0]
    rows = S // facets
    groups, tall, inside = split(facets)

    def sample_of(place):
        owner = place // rows
        within = place % rows
        group = owner // (facets // groups)
        line = (owner % (facets // groups)) * inside + within // tall
        return (within % tall + tall * group) * TILE + line

    blocks = S // 8
    inner = row_start + (NTOT // L) * sample_of(lax.broadcasted_iota(I32, (8, W), 0))
    outer = (NTOT // L) * sample_of(8 * lax.broadcasted_iota(I32, (blocks, W), 0))
    factors = {}

    def factor_tables(n, column, wide_column, scale):
        cosine, sine = cos_sin(mod_phase(inner, column))
        factors[n] = (cosine * scale, sine * scale)
        cosine, sine = cos_sin(mod_phase(outer, wide_column))
        outside[2 * n] = cosine
        outside[2 * n + 1] = sine

    def factor(n, k):
        cosine, sine = outside[2 * n, k : k + 1, :], outside[2 * n + 1, k : k + 1, :]
        x, y = factors[n]
        return x * cosine - y * sine, y * cosine + x * sine

    factor_tables(
        0,
        lax.broadcasted_iota(I32, (8, W), 1),
        lax.broadcasted_iota(I32, (blocks, W), 1),
        1.0 / math.sqrt(L),
    )
    factor_tables(1, W, W, 1.0)
    factor_tables(2, chunk, chunk, 1.0)
    for k in range(blocks):
        c1, s1 = factor(0, k)
        turn_c, turn_s = factor(1, k)
        twice = turn_c + turn_c
        for local in range(chunk // W):
            if local == 1:
                c0, s0 = c1, s1
                c1, s1 = c0 * turn_c - s0 * turn_s, s0 * turn_c + c0 * turn_s
            elif local:
                c0, c1 = c1, twice * c1 - c0
                s0, s1 = s1, twice * s1 - s0
            at = slice(local * W, (local + 1) * W)
            table[8 * k : 8 * k + 8, at] = c1.astype(BF16)
            table[S + 8 * k : S + 8 * k + 8, at] = s1.astype(BF16)
    for n in reversed(range(steps)):
        copies[n].wait()
        if n == 0:
            notes[0].wait()
            col_start = small[0][0, 0] + lax.axis_index("col") * count
            factor_tables(3, col_start, col_start, 1.0)
        part = slice(n * chunk, (n + 1) * chunk)
        cells = jnp.concatenate([held[0, part, :], held[1, part, :]], axis=1)
        upper = jnp.dot(table[0:S, :], cells, preferred_element_type=F32)
        lower = jnp.dot(table[S : 2 * S, :], cells, preferred_element_type=F32)
        for k in range(blocks):
            at = slice(8 * k, 8 * k + 8)
            re = upper[at, 0:W] + lower[at, W : 2 * W]
            im = upper[at, W : 2 * W] - lower[at, 0:W]
            if n + 1 < steps:
                old_re, old_im = total[at, 0:W], total[at, W : 2 * W]
                leap_c, leap_s = factor(2, k)
                re = re + (old_re * leap_c + old_im * leap_s)
                im = im + (old_im * leap_c - old_re * leap_s)
            if n == 0:
                turn_c, turn_s = factor(3, k)
                re, im = re * turn_c + im * turn_s, im * turn_c - re * turn_s
            total[at, 0:W] = re
            total[at, W : 2 * W] = im
    notes[1].wait()
    across = small[0][0, 1]
    spot = lax.broadcasted_iota(I32, (2, W), 1)
    note = jnp.where(spot == W - 2, across >> 8, jnp.where(spot == W - 1, across & 255, 0))
    for j in range(slots):
        note = jnp.where(spot == j, small[1][0, 0, j], note)
    note = note.astype(F32).astype(BF16)
    for o in range(facets):
        re = total[o * rows : (o + 1) * rows, 0:W].astype(BF16)
        im = total[o * rows : (o + 1) * rows, W : 2 * W].astype(BF16)
        for c in range(cols):
            at = (o * cols + c) * (2 * rows + 2)
            out[at : at + rows, :] = re
            out[at + rows : at + 2 * rows, :] = im
            out[at + 2 * rows : at + 2 * rows + 2, :] = note


def along(strip, row_offsets, facet_offsets, names, facets, cols):
    count = strip.shape[1]
    chunk = min(CHUNK, count)
    rows = S // facets
    return pl.pallas_call(
        functools.partial(along_kernel, facets, cols, chunk),
        out_shape=jax.ShapeDtypeStruct((facets * cols * (2 * rows + 2), W), BF16),
        in_specs=[pl.BlockSpec(memory_space=pltpu.SMEM)]
        + [pl.BlockSpec(memory_space=pltpu.HBM)] * 3,
        out_specs=pl.BlockSpec(memory_space=pltpu.VMEM),
        scratch_shapes=[
            pltpu.VMEM((2, count, W), BF16),
            pltpu.VMEM((2 * S, chunk), BF16),
            pltpu.VMEM((S, 2 * W), F32),
            pltpu.VMEM((8, S // 8, W), F32),
            [
                pltpu.SMEM(facet_offsets.shape, I32),
                pltpu.SMEM(names.shape, I32),
            ],
            pltpu.SemaphoreType.DMA((count // chunk + 2,)),
        ],
        cost_estimate=pl.CostEstimate(
            flops=8 * S * W * count, bytes_accessed=4 * count * W, transcendentals=0
        ),
        name="along",
    )(row_offsets, facet_offsets, names, strip)


def base_kernel(columns, out):
    cell = lax.broadcasted_iota(I32, (W, 2 * S), 0)
    lane = lax.broadcasted_iota(I32, (W, 2 * S), 1)
    turn = ((lane >> 5) & 1) * (NTOT // 4)
    top, bottom = cos_sin((cell * positions(columns[0], lane) + turn) & (NTOT - 1))
    scale = 1.0 / math.sqrt(W)
    out[0:W, :] = (top * scale).astype(BF16)
    out[W : 2 * W, :] = (bottom * scale).astype(BF16)


def positions(column, lane):
    return column + (NTOT // S) * ((lane >> 6) * TILE + (lane & (TILE - 1)))


def base(columns):
    return pl.pallas_call(
        base_kernel,
        out_shape=jax.ShapeDtypeStruct((2 * W, 2 * S), BF16),
        in_specs=[pl.BlockSpec(memory_space=pltpu.SMEM)],
        out_specs=pl.BlockSpec(memory_space=pltpu.VMEM),
        compiler_params=pltpu.CompilerParams(vmem_limit_bytes=VMEM_LIMIT),
        cost_estimate=pl.CostEstimate(flops=1 << 24, bytes_accessed=1 << 18, transcendentals=0),
        name="base",
    )(columns)


def across_kernel(facets, cols, columns, got, right, out, left, summed, phases):
    rows = S // facets
    groups, tall, inside = split(facets)
    slots = out.shape[1]
    wide = 2 * S
    height = facets * rows
    size = 2 * rows + 2
    column = lax.axis_index("col")
    sources = []
    for f in range(facets):
        for h in range(cols):
            at = (f * cols + h) * size
            re, im = got[at : at + rows, :], got[at + rows : at + 2 * rows, :]
            near, far = slice(2 * h * W, (2 * h + 1) * W), slice((2 * h + 1) * W, (2 * h + 2) * W)
            left[f * rows : (f + 1) * rows, near] = re
            left[f * rows : (f + 1) * rows, far] = im
            left[height + f * rows : height + (f + 1) * rows, near] = im
            left[height + f * rows : height + (f + 1) * rows, far] = -re
        note = None
        for h in range(cols):
            at = (f * cols + h) * size + 2 * rows
            value = jnp.where(column == h, got[at : at + 2, :].astype(F32)[0:1], 0.0)
            note = value if note is None else note + value
        sources.append(note)
    table = jnp.concatenate([right[...]] * cols, axis=0)
    summed[...] = jnp.dot(left[...], table, preferred_element_type=F32)
    heads = jnp.concatenate(sources, axis=0)
    offset = (heads[:, W - 2 : W - 1] * 256.0 + heads[:, W - 1 : W]).astype(I32)
    lane = lax.broadcasted_iota(I32, (facets, wide), 1)
    cosine, sine = cos_sin(mod_phase(offset, positions(columns[0], lane)))
    phases[0] = cosine
    phases[1] = sine
    acc = jnp.zeros((rows, wide), F32)
    for f in range(facets):
        acc = acc + summed[f * rows : (f + 1) * rows, :] * phases[0, f : f + 1, :]
        acc = acc + summed[height + f * rows : height + (f + 1) * rows, :] * phases[1, f : f + 1, :]
    acc = acc * (1.0 / math.sqrt(facets))
    pieces = []
    for b in range(S // TILE):
        at = slice(b * 2 * TILE, (b + 1) * 2 * TILE)
        parts = [acc[i * tall : (i + 1) * tall, at] for i in range(inside)]
        if inside == 1:
            parts.append(jnp.zeros_like(parts[0]))
        pieces.append(jnp.concatenate(parts, axis=1))
    tiles = jnp.concatenate(pieces, axis=0).astype(BF16)
    line = lax.broadcasted_iota(I32, (facets * slots, facets), 0)
    place = line - slots * lax.broadcasted_iota(I32, line.shape, 1)
    owner = jnp.where((place >= 0) & (place < slots), 1.0, 0.0)
    spread = jnp.dot(owner.astype(BF16), heads.astype(BF16), preferred_element_type=F32)
    line = lax.broadcasted_iota(I32, spread.shape, 0)
    own = lax.broadcasted_iota(I32, spread.shape, 1) == (line & (slots - 1))
    names = jnp.sum(jnp.where(own, spread, 0.0), axis=1, keepdims=True).astype(I32)
    first = (lax.axis_index("facet") // (facets // groups)) * tall
    local = (names >> 3) - first
    wanted = jnp.where((local >= 0) & (local < tall), (names & 7) * tall + local, -1)
    count = tiles.shape[0]
    spot = lax.broadcasted_iota(I32, (facets * slots, W), 1)
    onehot = jnp.where(wanted == spot, 1.0, 0.0).astype(BF16)[:, 0:count]
    chosen = jnp.dot(onehot, tiles, preferred_element_type=F32)
    for o in range(facets):
        out[o] = chosen[o * slots : (o + 1) * slots, :].astype(BF16)


def across(got, right, columns, slots, facets, cols):
    return pl.pallas_call(
        functools.partial(across_kernel, facets, cols),
        out_shape=jax.ShapeDtypeStruct((facets, slots, W), BF16),
        in_specs=[
            pl.BlockSpec(memory_space=pltpu.SMEM),
            pl.BlockSpec(memory_space=pltpu.VMEM),
            pl.BlockSpec(memory_space=pltpu.VMEM),
        ],
        out_specs=pl.BlockSpec(memory_space=pltpu.VMEM),
        scratch_shapes=[
            pltpu.VMEM((2 * S, 2 * W * cols), BF16),
            pltpu.VMEM((2 * S, 2 * S), F32),
            pltpu.VMEM((2, facets, 2 * S), F32),
        ],
        compiler_params=pltpu.CompilerParams(vmem_limit_bytes=VMEM_LIMIT),
        cost_estimate=pl.CostEstimate(
            flops=2 * 2 * S * 2 * W * 2 * S, bytes_accessed=1 << 20, transcendentals=0
        ),
        name="across",
    )(columns, got, right)


def waves_kernel(facets, live, uv, right, near, far):
    _, _, inside = split(facets)
    vis = uv.shape[2]
    step = NTOT // UV_STEPS
    line = lax.broadcasted_iota(I32, (TILE, vis), 0)
    low = line[0:8] * inside
    high = (line[0:4] % (4 // inside)) * 8 * inside + line[0:4] // (4 // inside)

    def slot(j, carry):
        cosine, sine = cos_sin((uv[j, 1:2, :] * (line * step)) & (NTOT - 1))
        cos_high, sin_high = cosine.astype(BF16), sine.astype(BF16)
        right[j, 0:TILE, :] = cos_high
        right[j, TILE : 2 * TILE, :] = sin_high
        right[j, 2 * TILE : 3 * TILE, :] = (cosine - cos_high.astype(F32)).astype(BF16)
        right[j, 3 * TILE : 4 * TILE, :] = (sine - sin_high.astype(F32)).astype(BF16)
        cosine, sine = cos_sin((uv[j, 0:1, :] * (low * step)) & (NTOT - 1))
        size = jnp.where(j < live[0, 0], 1.0 / TILE, 0.0)
        near[j, 0] = cosine * size
        near[j, 1] = sine * size
        cosine, sine = cos_sin((uv[j, 0:1, :] * (high * step)) & (NTOT - 1))
        far[j, 0] = cosine
        far[j, 1] = sine
        return carry

    lax.fori_loop(0, uv.shape[0], slot, 0)


def waves(live, uv, facets):
    slots, _, vis = uv.shape
    return pl.pallas_call(
        functools.partial(waves_kernel, facets),
        out_shape=(
            jax.ShapeDtypeStruct((slots, 4 * TILE, vis), BF16),
            jax.ShapeDtypeStruct((slots, 2, 8, vis), F32),
            jax.ShapeDtypeStruct((slots, 2, 4, vis), F32),
        ),
        in_specs=[
            pl.BlockSpec(memory_space=pltpu.SMEM),
            pl.BlockSpec(memory_space=pltpu.VMEM),
        ],
        out_specs=[pl.BlockSpec(memory_space=pltpu.VMEM)] * 3,
        compiler_params=pltpu.CompilerParams(vmem_limit_bytes=VMEM_LIMIT),
        cost_estimate=pl.CostEstimate(flops=1 << 26, bytes_accessed=3 << 20, transcendentals=0),
        name="waves",
    )(live, uv)


def visibility_kernel(facets, parts, right, near, far, out, held):
    groups, _, inside = split(facets)
    slots, vis = out.shape[0], out.shape[2]
    sources = facets // groups
    for f in range(sources):
        held[f] = parts[f].astype(F32)
        for g in range(1, groups):
            held[f] += parts[g * sources + f].astype(F32)
    lane = lax.broadcasted_iota(I32, (sources, W), 1)
    sign = jnp.where((lane & TILE) == 0, 1.0, -1.0).astype(F32)
    for j in range(slots):
        x = held[:, j, :]
        y = pltpu.roll(x, W // 2, 1)
        both = [jnp.where(lane < W // 2, x, y), jnp.where(lane < W // 2, y, x)][:inside]
        lhs = [z * sign for z in both] + [pltpu.roll(z, TILE, 1) for z in both]
        lhs = jnp.concatenate(lhs, axis=0).astype(BF16)
        for at in range(0, vis, vis // 2):
            cut = slice(at, at + vis // 2)
            middle = jnp.dot(lhs, right[j, :, cut], preferred_element_type=F32)
            real, imag = middle[0:8], middle[TILE : TILE + 8]
            for h in range(1, 4):
                more_re = middle[8 * h : 8 * h + 8]
                more_im = middle[TILE + 8 * h : TILE + 8 * h + 8]
                cosine, sine = far[j, 0, h : h + 1, cut], far[j, 1, h : h + 1, cut]
                real = real + (cosine * more_re - sine * more_im)
                imag = imag + (cosine * more_im + sine * more_re)
            cosine, sine = near[j, 0, :, cut], near[j, 1, :, cut]
            out[j, 0:1, cut] = jnp.sum(cosine * real - sine * imag, axis=0, keepdims=True)
            out[j, 1:2, cut] = jnp.sum(cosine * imag + sine * real, axis=0, keepdims=True)


def visibilities_of(parts, tables, facets):
    slots, _, vis = tables[0].shape
    return pl.pallas_call(
        functools.partial(visibility_kernel, facets),
        out_shape=jax.ShapeDtypeStruct((slots, 2, vis), F32),
        in_specs=[pl.BlockSpec(memory_space=pltpu.VMEM)] * 4,
        out_specs=pl.BlockSpec(memory_space=pltpu.VMEM),
        scratch_shapes=[pltpu.VMEM((facets // split(facets)[0], slots, W), F32)],
        compiler_params=pltpu.CompilerParams(vmem_limit_bytes=VMEM_LIMIT),
        cost_estimate=pl.CostEstimate(
            flops=slots * 2 * 64 * 128 * vis, bytes_accessed=1 << 20, transcendentals=0
        ),
        name="visibility",
    )(parts, *tables)


def shards(
    facet_strips, facet_offsets, column_offsets, row_offsets, tile_lists, tile_counts, uv_index
):
    facets, cols = lax.axis_size("facet"), lax.axis_size("col")
    sent = along(facet_strips[0], row_offsets, facet_offsets, tile_lists, facets, cols)
    pairs = sent.reshape((facets * cols, -1, 2, W))
    got = lax.all_to_all(pairs, ("facet", "col"), 0, 0, tiled=True)
    got = got.reshape(sent.shape)
    right = base(column_offsets)
    tables = waves(tile_counts, uv_index[0, 0], facets)
    asked = across(got, right, column_offsets, tile_lists.shape[2], facets, cols)
    parts = lax.all_to_all(asked, "facet", 0, 0, tiled=True)
    result = visibilities_of(parts, tables, facets)
    return result[None, None]


def solution(mesh):
    in_specs = (
        P("facet", None, "col", None),
        P("facet", None),
        P("col"),
        P(),
        P("col", "facet", None),
        P("col", "facet"),
        P("col", "facet", None, None, None),
    )
    out_specs = P("col", "facet", None, None, None)
    return jax.shard_map(shards, mesh=mesh, in_specs=in_specs, out_specs=out_specs, check_vma=False)
```
